16 devices in a mesh: dp: 4 (over z, y), tp: 4 (over x, core).
Axes of the slice: x: 2, y: 2, z: 2, core: 2. Of those that a mesh axis runs over, the one named last changes fastest.
Arguments:
- hidden: bfloat16 [4, 128, 5120], P('dp', 'tp'), parts along dimension 0
- vision: bfloat16 [4, 512, 5120], P('dp', 'tp'), parts along dimension 0
- positions: int32 [4, 128], P('dp', 'tp'), parts along dimension 0
- tile_mask: int32 [4, 128, 4], P('dp', 'tp'), parts along dimension 0
- ln1_a: bfloat16 [5120], replicated
- wq_a: bfloat16 [5120, 5120], P(None, 'tp')
- wk_a: bfloat16 [5120, 1024], P(None, 'tp')
- wv_a: bfloat16 [5120, 1024], P(None, 'tp')
- wo_a: bfloat16 [5120, 5120], P('tp')
- ln2_a: bfloat16 [5120], replicated
- wg_a: bfloat16 [5120, 13824], P(None, 'tp')
- wu_a: bfloat16 [5120, 13824], P(None, 'tp')
- wd_a: bfloat16 [13824, 5120], P('tp')
- ln1_b: bfloat16 [5120], replicated
- wq_b: bfloat16 [5120, 5120], P(None, 'tp')
- q_norm: bfloat16 [128], replicated
- wk_b: bfloat16 [5120, 1024], P(None, 'tp')
- wv_b: bfloat16 [5120, 1024], P(None, 'tp')
- k_norm: bfloat16 [128], replicated
- wo_b: bfloat16 [5120, 5120], P('tp')
- ln2_b: bfloat16 [5120], replicated
- wg_b: bfloat16 [5120, 13824], P(None, 'tp')
- wu_b: bfloat16 [5120, 13824], P(None, 'tp')
- wd_b: bfloat16 [13824, 5120], P('tp')
- xgates: float32 [2], replicated
Outputs:
- output: bfloat16 [4, 128, 5120], P('dp', 'tp'), parts along dimension 0
There are 4 independent parts. The reference program is written for one: setup_inputs(seed, part) draws one part's arguments, and reference() takes and returns one part's arrays. A program takes and returns all parts, laid end to end along the dimension named above; an argument that names none is the same for every part.
All inputs are finite; a program needn't handle non-finite values.
Results may differ from the reference program's by a relative error of at most 0.015711.
Values are sent between devices in bfloat16 or wider.
A program may use at most 1.25 GiB of HBM per device.

```python
import math
import jax
import jax.numpy as jnp
from jax import lax

SAMPLES = 1
TOKENS = 128
VISION_TOKENS = 512
MODEL_DIM = 5120
NUM_HEADS = 40
KV_HEADS = 8
HEAD_DIM = 128
FFN_DIM = 13824
NUM_TILES = 4

ROPE_THETA = 500000.0
ROPE_FACTOR = 8.0
LOW_FACTOR = 1.0
HIGH_FACTOR = 4.0
ORIG_CONTEXT = 8192.0
NORM_EPS = 1e-5
MASK_VALUE = -1e30


def rope_table(head_dim):
    low_wave = ORIG_CONTEXT / LOW_FACTOR
    high_wave = ORIG_CONTEXT / HIGH_FACTOR
    freq_list = []
    for freq_idx in range(head_dim // 2):
        base_freq = 1.0 / (ROPE_THETA ** (2.0 * freq_idx / head_dim))
        wave_len = 2.0 * math.pi / base_freq
        if wave_len > low_wave:
            freq_list.append(base_freq / ROPE_FACTOR)
        elif wave_len < high_wave:
            freq_list.append(base_freq)
        else:
            smooth = (ORIG_CONTEXT / wave_len - LOW_FACTOR) / (HIGH_FACTOR - LOW_FACTOR)
            freq_list.append((1.0 - smooth) * base_freq / ROPE_FACTOR + smooth * base_freq)
    return jnp.array(freq_list, dtype=jnp.float32)


def rms_scale(values, norm_gain):
    values = values.astype(jnp.float32)
    mean_sq = jnp.mean(values * values, axis=-1, keepdims=True)
    return values * lax.rsqrt(mean_sq + NORM_EPS) * norm_gain.astype(jnp.float32)


def rotate(values, cos_tab, sin_tab):
    half_dim = values.shape[-1] // 2
    first_half = values[..., :half_dim]
    second_half = values[..., half_dim:]
    return jnp.concatenate([first_half * cos_tab - second_half * sin_tab, second_half * cos_tab + first_half * sin_tab], axis=-1)


def group_attention(queries, key_vecs, val_vecs, allowed):
    def one_group(operands):
        query_grp, key_grp, val_grp = operands
        scores = jnp.einsum('rqd,kd->rqk', query_grp.astype(jnp.float32), key_grp.astype(jnp.float32)) * (HEAD_DIM ** -0.5)
        weights = jax.nn.softmax(jnp.where(allowed[None], scores, MASK_VALUE), axis=-1).astype(jnp.bfloat16)
        return jnp.einsum('rqk,kd->rqd', weights.astype(jnp.float32), val_grp.astype(jnp.float32)).astype(jnp.bfloat16)
    grouped = lax.map(one_group, (jnp.transpose(queries, (1, 2, 0, 3)), jnp.transpose(key_vecs, (1, 0, 2)), jnp.transpose(val_vecs, (1, 0, 2))))
    return jnp.transpose(grouped, (2, 0, 1, 3)).reshape(queries.shape[0], -1)


def gated_mlp(resid, norm_gain, w_gate, w_up, w_down):
    normed = rms_scale(resid, norm_gain).astype(jnp.bfloat16)
    gate_proj = jnp.dot(normed, w_gate, preferred_element_type=jnp.float32)
    up_proj = jnp.dot(normed, w_up, preferred_element_type=jnp.float32)
    activated = (jax.nn.silu(gate_proj) * up_proj).astype(jnp.bfloat16)
    return jnp.dot(activated, w_down, preferred_element_type=jnp.float32)


def setup_inputs(seed: int = 0, part: int = 0) -> dict:
    data_keys = jax.random.split(jax.random.fold_in(jax.random.key(seed + 1), part), 6)
    weight_keys = jax.random.split(jax.random.key(seed), 22)
    qk_scale = max(math.log(TOKENS / 8.0), 1.0) ** 0.25
    cross_gain = max(math.log(VISION_TOKENS / 16.0), 1.0) ** 0.25
    q_width = NUM_HEADS * HEAD_DIM
    kv_width = KV_HEADS * HEAD_DIM
    dim_scale = MODEL_DIM ** -0.5

    def draw_normal(key_val, arr_shape, spread):
        return (jax.random.normal(key_val, arr_shape, jnp.float32) * spread).astype(jnp.bfloat16)

    def draw_gain(key_val, arr_shape, center):
        return (center * (1.0 + 0.2 * jax.random.normal(key_val, arr_shape, jnp.float32))).astype(jnp.bfloat16)

    hidden = draw_normal(data_keys[0], (SAMPLES, TOKENS, MODEL_DIM), 1.0)
    vision = draw_normal(data_keys[1], (SAMPLES, VISION_TOKENS, MODEL_DIM), 1.0)
    pos_steps = jax.random.randint(data_keys[2], (SAMPLES, TOKENS), 1, 4, dtype=jnp.int32)
    offsets = jax.random.randint(data_keys[3], (SAMPLES, 1), 0, TOKENS, dtype=jnp.int32)
    positions = (offsets + jnp.cumsum(pos_steps, axis=1)).astype(jnp.int32)
    begins = jax.random.randint(data_keys[4], (SAMPLES, 1, 1), 0, TOKENS // 4 + 1, dtype=jnp.int32)
    tile_bits = jax.random.randint(data_keys[5], (SAMPLES, TOKENS, NUM_TILES), 0, 2, dtype=jnp.int32)
    tile_mask = jnp.where(jnp.arange(TOKENS, dtype=jnp.int32)[None, :, None] >= begins, tile_bits, 0).astype(jnp.int32)
    magnitudes = jax.random.uniform(weight_keys[20], (2,), jnp.float32, 0.6, 1.4)
    gate_signs = (2 * jax.random.randint(weight_keys[21], (2,), 0, 2, dtype=jnp.int32) - 1).astype(jnp.float32)
    return {
        'hidden': hidden,
        'vision': vision,
        'positions': positions,
        'tile_mask': tile_mask,
        'ln1_a': draw_gain(weight_keys[0], (MODEL_DIM,), 1.0),
        'wq_a': draw_normal(weight_keys[1], (MODEL_DIM, q_width), qk_scale * dim_scale),
        'wk_a': draw_normal(weight_keys[2], (MODEL_DIM, kv_width), qk_scale * dim_scale),
        'wv_a': draw_normal(weight_keys[3], (MODEL_DIM, kv_width), dim_scale),
        'wo_a': draw_normal(weight_keys[4], (q_width, MODEL_DIM), q_width ** -0.5),
        'ln2_a': draw_gain(weight_keys[5], (MODEL_DIM,), 1.0),
        'wg_a': draw_normal(weight_keys[6], (MODEL_DIM, FFN_DIM), dim_scale),
        'wu_a': draw_normal(weight_keys[7], (MODEL_DIM, FFN_DIM), dim_scale),
        'wd_a': draw_normal(weight_keys[8], (FFN_DIM, MODEL_DIM), FFN_DIM ** -0.5),
        'ln1_b': draw_gain(weight_keys[9], (MODEL_DIM,), 1.0),
        'wq_b': draw_normal(weight_keys[10], (MODEL_DIM, q_width), dim_scale),
        'q_norm': draw_gain(weight_keys[11], (HEAD_DIM,), cross_gain),
        'wk_b': draw_normal(weight_keys[12], (MODEL_DIM, kv_width), dim_scale),
        'wv_b': draw_normal(weight_keys[13], (MODEL_DIM, kv_width), dim_scale),
        'k_norm': draw_gain(weight_keys[14], (HEAD_DIM,), cross_gain),
        'wo_b': draw_normal(weight_keys[15], (q_width, MODEL_DIM), q_width ** -0.5),
        'ln2_b': draw_gain(weight_keys[16], (MODEL_DIM,), 1.0),
        'wg_b': draw_normal(weight_keys[17], (MODEL_DIM, FFN_DIM), dim_scale),
        'wu_b': draw_normal(weight_keys[18], (MODEL_DIM, FFN_DIM), dim_scale),
        'wd_b': draw_normal(weight_keys[19], (FFN_DIM, MODEL_DIM), FFN_DIM ** -0.5),
        'xgates': magnitudes * gate_signs,
    }


def reference(hidden, vision, positions, tile_mask, ln1_a, wq_a, wk_a, wv_a, wo_a, ln2_a, wg_a, wu_a, wd_a, ln1_b, wq_b, q_norm, wk_b, wv_b, k_norm, wo_b, ln2_b, wg_b, wu_b, wd_b, xgates):
    rep_heads = NUM_HEADS // KV_HEADS
    tile_len = VISION_TOKENS // NUM_TILES
    inv_freq = rope_table(HEAD_DIM)
    gate_vals = jnp.tanh(xgates.astype(jnp.float32))
    causal = lax.broadcasted_iota(jnp.int32, (TOKENS, TOKENS), 0) >= lax.broadcasted_iota(jnp.int32, (TOKENS, TOKENS), 1)

    def one_sample(operands):
        hid_rows, vis_rows, pos_row, mask_row = operands
        angles = pos_row.astype(jnp.float32)[:, None] * inv_freq[None, :]
        cos_tab = jnp.cos(angles)[:, None, :]
        sin_tab = jnp.sin(angles)[:, None, :]
        normed = rms_scale(hid_rows, ln1_a).astype(jnp.bfloat16)
        queries = jnp.dot(normed, wq_a, preferred_element_type=jnp.float32).reshape(TOKENS, NUM_HEADS, HEAD_DIM)
        queries = rotate(queries, cos_tab, sin_tab).astype(jnp.bfloat16).reshape(TOKENS, KV_HEADS, rep_heads, HEAD_DIM)
        key_vecs = jnp.dot(normed, wk_a, preferred_element_type=jnp.float32).reshape(TOKENS, KV_HEADS, HEAD_DIM)
        key_vecs = rotate(key_vecs, cos_tab, sin_tab).astype(jnp.bfloat16)
        val_vecs = jnp.dot(normed, wv_a, preferred_element_type=jnp.float32).astype(jnp.bfloat16).reshape(TOKENS, KV_HEADS, HEAD_DIM)
        context = group_attention(queries, key_vecs, val_vecs, causal)
        h_one = (hid_rows.astype(jnp.float32) + jnp.dot(context, wo_a, preferred_element_type=jnp.float32)).astype(jnp.bfloat16)
        h_two = (h_one.astype(jnp.float32) + gated_mlp(h_one, ln2_a, wg_a, wu_a, wd_a)).astype(jnp.bfloat16)
        normed = rms_scale(h_two, ln1_b).astype(jnp.bfloat16)
        queries = jnp.dot(normed, wq_b, preferred_element_type=jnp.float32).reshape(TOKENS, NUM_HEADS, HEAD_DIM)
        queries = rms_scale(queries, q_norm).astype(jnp.bfloat16).reshape(TOKENS, KV_HEADS, rep_heads, HEAD_DIM)
        key_vecs = jnp.dot(vis_rows, wk_b, preferred_element_type=jnp.float32).reshape(VISION_TOKENS, KV_HEADS, HEAD_DIM)
        key_vecs = rms_scale(key_vecs, k_norm).astype(jnp.bfloat16)
        val_vecs = jnp.dot(vis_rows, wv_b, preferred_element_type=jnp.float32).astype(jnp.bfloat16).reshape(VISION_TOKENS, KV_HEADS, HEAD_DIM)
        visible = mask_row > 0
        allowed = jnp.repeat(visible, tile_len, axis=1)
        context = group_attention(queries, key_vecs, val_vecs, allowed)
        row_keep = jnp.any(visible, axis=-1, keepdims=True).astype(jnp.float32)
        attn_out = jnp.dot(context, wo_b, preferred_element_type=jnp.float32)
        h_three = (h_two.astype(jnp.float32) + gate_vals[0] * row_keep * attn_out).astype(jnp.bfloat16)
        mlp_out = gated_mlp(h_three, ln2_b, wg_b, wu_b, wd_b)
        return (h_three.astype(jnp.float32) + gate_vals[1] * row_keep * mlp_out).astype(jnp.bfloat16)

    return lax.map(one_sample, (hidden, vision, positions, tile_mask))
```

```python
import functools
import math

import jax
import jax.numpy as jnp
from jax import lax
from jax.experimental import pallas as pl
from jax.experimental.pallas import tpu as pltpu
from jax.sharding import PartitionSpec as P

ROPE_THETA = 500000.0
ROPE_FACTOR = 8.0
LOW_FACTOR = 1.0
HIGH_FACTOR = 4.0
ORIG_CONTEXT = 8192.0
NORM_EPS = 1e-5
MASK_VALUE = -1e30
MESH = pl.DeviceIdType.MESH
F32 = jnp.float32
BF16 = jnp.bfloat16

D = 5120
TOK = 128
HD = 128
HEADS = 10
GROUPS = 2
REP = 5
FF = 3456
TILES = 4
CH = 10
CW = D // CH
HW = CW // 2
UNIT = 128
RING = 1440
AGC = 4
VCH = 8
VROWS = TOK // VCH

SEG = {
    "qkv_a": (0, 560, 1),
    "o_a": (560, 40, 10),
    "gu_a": (960, 80, 27),
    "d_a": (3120, 120, 10),
    "kv_b": (4320, 160, 1),
    "q_b": (4480, 40, 10),
    "o_b": (4880, 40, 10),
    "gu_b": (5280, 80, 27),
    "d_b": (7440, 120, 10),
}
SEMS = {"qkv_a": 0, "o_a": 2, "gu_a": 12, "d_a": 21, "kv_b": 31, "q_b": 32, "o_b": 34, "gu_b": 44, "d_b": 53}
NSEM = 63


def rope_table(head_dim):
    low_wave = ORIG_CONTEXT / LOW_FACTOR
    high_wave = ORIG_CONTEXT / HIGH_FACTOR
    freq_list = []
    for freq_idx in range(head_dim // 2):
        base_freq = 1.0 / (ROPE_THETA ** (2.0 * freq_idx / head_dim))
        wave_len = 2.0 * math.pi / base_freq
        if wave_len > low_wave:
            freq_list.append(base_freq / ROPE_FACTOR)
        elif wave_len < high_wave:
            freq_list.append(base_freq)
        else:
            smooth = (ORIG_CONTEXT / wave_len - LOW_FACTOR) / (HIGH_FACTOR - LOW_FACTOR)
            freq_list.append((1.0 - smooth) * base_freq / ROPE_FACTOR + smooth * base_freq)
    return jnp.array(freq_list, dtype=jnp.float32)


def head_norm(values, gain):
    mean_sq = jnp.mean(values * values, axis=-1, keepdims=True)
    return values * lax.rsqrt(mean_sq + NORM_EPS) * gain


def softmax_rows(scores):
    top = jnp.max(scores, axis=-1, keepdims=True)
    weights = jnp.exp(scores - top)
    return (weights / jnp.sum(weights, axis=-1, keepdims=True)).astype(BF16)


def dot_nt(left, right):
    return lax.dot_general(left, right, (((1,), (1,)), ((), ())), preferred_element_type=F32)


def kernel(pos, tmask, gains, small, hid, vis, wq_a, wk_a, wv_a, wo_a, wg_a, wu_a, wd_a, wq_b, wk_b, wv_b, wo_b, wg_b, wu_b, wd_b, out,
           ring, hbuf, xn, vbuf, meta, cos_s, sin_s, fac, qs, ks, vs, kb, vb, ctx, act, pall, psib, csum, crcv, ostage, fin,
           wsem, lsem, ag_s, ag_r, mt_s, mt_r, vx_s, vx_r, vr_s, vr_r, vo_s, vo_r, ps_s, ps_r, cs_s, cs_r, hh_s, hh_r):
    me = lax.axis_index("tp")
    xi = lax.div(me, 2)
    co = lax.rem(me, 2)
    sib = xi * 2 + 1 - co
    cross = (1 - xi) * 2 + co
    diag = (1 - xi) * 2 + 1 - co

    def remote(src, dst, ssem, rsem, dev):
        return pltpu.make_async_remote_copy(src_ref=src, dst_ref=dst, send_sem=ssem, recv_sem=rsem, device_id={"tp": dev}, device_id_type=MESH)

    def spot(name, j):
        first, units, _ = SEG[name]
        return lax.rem(first + j * units, RING) * UNIT

    def put(weight, rows, col, at, sem):
        pltpu.make_async_copy(weight.at[:, pl.ds(pl.multiple_of(col * 128, 128), 128)], ring.at[pl.ds(pl.multiple_of(at, 128), rows)], sem).start()

    def start_group(name, j):
        at = spot(name, j)
        base = SEMS[name]
        if name[:2] == "o_":
            for p in range(4):
                put(wo_a if name == "o_a" else wo_b, 1280, j * 4 + p, at + p * 1280, wsem.at[base + j])
        elif name[:2] == "gu":
            sem = wsem.at[base + lax.div(j, 3)]
            put(wg_a if name == "gu_a" else wg_b, D, j, at, sem)
            put(wu_a if name == "gu_a" else wu_b, D, j, at + D, sem)
        elif name[:2] == "d_":
            for p in range(4):
                put(wd_a if name == "d_a" else wd_b, FF, j * 4 + p, at + p * 30 * UNIT, wsem.at[base + j])
        elif name == "q_b":
            put(wq_b, D, j, at, wsem.at[base + lax.div(j, 8)])
        elif name == "kv_b":
            for p, w in enumerate((wk_b, wk_b, wv_b, wv_b)):
                put(w, D, p % 2, at + p * D, wsem.at[base])
        else:
            for p in range(14):
                w = wq_a if p < 10 else (wk_a if p < 12 else wv_a)
                put(w, D, p if p < 10 else p % 2, at + p * D, wsem.at[base + p // 8])

    def ready(name, freed):
        first, units, count = SEG[name]
        if isinstance(freed, int):
            return min(max((freed + RING - first) // units, 0), count)
        return jnp.minimum(jnp.maximum(lax.div(freed + RING - first + 100 * units, units) - 100, 0), count)

    def refill(before, after, low, high):
        for name, (first, units, count) in SEG.items():
            if first + units > high + RING or first + units * count <= low + RING:
                continue
            lo, hi = ready(name, before), ready(name, after)
            if isinstance(lo, int) and isinstance(hi, int) and lo >= hi:
                continue
            lax.fori_loop(lo, hi, lambda j, _, name=name: (start_group(name, j), 0)[1], 0)

    def landed(at, rows, sem):
        span = ring.at[pl.ds(pl.multiple_of(at, 128), rows)]
        pltpu.make_async_copy(span, span, sem).wait()

    def panels(at, rows, pitch, count):
        return jnp.concatenate([ring[pl.ds(pl.multiple_of(at + p * pitch, 128), rows), :] for p in range(count)], axis=1)

    def mm(left, right):
        return jnp.dot(left, right, preferred_element_type=F32)

    own_rows = pl.ds(pl.multiple_of(me * 32, 32), 32)
    load_h = pltpu.make_async_copy(hid.at[0], hbuf.at[own_rows], lsem.at[0])
    load_h.start()
    load_v = pltpu.make_async_copy(vis.at[0], vbuf.at[me], lsem.at[1])
    barrier = pltpu.get_barrier_semaphore()
    for dev in (sib, cross, diag):
        pl.semaphore_signal(barrier, inc=1, device_id={"tp": dev}, device_id_type=MESH)
    for name in SEG:
        for j in range(ready(name, 0) if name == "qkv_a" else 0):
            start_group(name, j)
    row_i = lax.broadcasted_iota(jnp.int32, (32, 128), 0)
    lane_i = lax.broadcasted_iota(jnp.int32, (32, 128), 1)
    pos_row = jnp.concatenate([jnp.broadcast_to(pos[...].astype(F32), (32, 32)), jnp.zeros((32, 96), F32)], axis=1)
    pos_col = jnp.sum(jnp.where(row_i == lane_i, pos_row, 0.0), axis=1, keepdims=True)
    own_meta = jnp.where(lane_i == 0, pos_col, 0.0)
    tm = tmask[0].astype(F32)
    for j in range(TILES):
        own_meta = jnp.where(lane_i == j + 1, tm[:, j:j + 1], own_meta)
    meta[own_rows, :] = own_meta
    load_h.wait()
    pl.semaphore_wait(barrier, 3)

    def ag(kind, k):
        cols = pl.ds(k * (D // AGC), D // AGC)
        rows = pl.ds(pl.multiple_of((cross if kind == 2 else me) * 32, 32), 32)
        ref = hbuf.at[rows, cols]
        return remote(ref, ref, ag_s.at[kind, k], ag_r.at[kind, k], cross if kind == 1 else sib)

    for k in range(AGC):
        ag(1, k).start()
    for k in range(AGC):
        ag(0, k).start()
    metas = [remote(meta.at[own_rows], meta.at[own_rows], mt_s.at[i], mt_r.at[i], dev) for i, dev in enumerate((sib, cross, diag))]
    for m in metas:
        m.start()
    load_v.start()
    refill(-RING, 0, 560 - RING, 0)

    def norm_rows(first, count, gain):
        def block(b, _):
            rows = pl.ds(pl.multiple_of(first + b * 16, 16), 16)
            v = hbuf[rows, :].astype(F32)
            scale = lax.rsqrt(jnp.mean(v * v, axis=-1, keepdims=True) + NORM_EPS)
            xn[rows, :] = (v * scale * gains[gain:gain + 1, :]).astype(BF16)
            return 0
        lax.fori_loop(0, count // 16, block, 0)

    norm_rows(me * 32, 32, 0)
    for k in range(AGC):
        ag(0, k).wait_recv()
    norm_rows(sib * 32, 32, 0)
    for m in metas:
        m.wait_recv()
    angles = meta[:, 0:1] * small[2:3, :]
    cos_s[...] = jnp.cos(angles)
    lanes = lax.broadcasted_iota(jnp.int32, (TOK, HD), 1)
    sin_s[...] = jnp.where(lanes < HD // 2, -jnp.sin(angles), jnp.sin(angles))
    keep = jnp.max(jnp.where((lanes >= 1) & (lanes <= TILES), meta[...], 0.0), axis=1, keepdims=True)
    fac[0] = jnp.broadcast_to(jnp.where(keep > 0.0, 1.0, 0.0) * small[3:4, 0:1], (TOK, HW))
    fac[1] = jnp.broadcast_to(jnp.where(keep > 0.0, 1.0, 0.0) * small[4:5, 0:1], (TOK, HW))
    for k in range(AGC):
        ag(1, k).wait_recv()
        ag(2, k).start()
    norm_rows(cross * 32, 32, 0)

    load_v.wait()

    def vown():
        return remote(vbuf.at[me], vbuf.at[me], vo_s, vo_r, sib)

    def vcross(k):
        ref = vbuf.at[me, pl.ds(k * VROWS, VROWS), :]
        return remote(ref, ref, vx_s.at[k], vx_r.at[k], cross)

    def vrelay(k):
        ref = vbuf.at[cross, pl.ds(k * VROWS, VROWS), :]
        return remote(ref, ref, vr_s.at[k], vr_r.at[k], sib)

    for k in range(0, 2):
        vcross(k).start()
    for k in range(AGC):
        ag(2, k).wait_recv()
    norm_rows(diag * 32, 32, 0)
    vown().start()

    def rope(v):
        return (v * cos_s[...] + pltpu.roll(v, HD // 2, 1) * sin_s[...]).astype(BF16)

    at = spot("qkv_a", 0)
    landed(at, 8 * D, wsem.at[0])
    r = mm(xn[...], panels(at, D, D, 8))
    for i in range(8):
        qs[i] = rope(r[:, i * HD:(i + 1) * HD])
    landed(at + 8 * D, 6 * D, wsem.at[1])
    r = mm(xn[...], panels(at + 8 * D, D, D, 6))
    for i in range(2):
        qs[8 + i] = rope(r[:, i * HD:(i + 1) * HD])
        ks[i] = rope(r[:, (2 + i) * HD:(3 + i) * HD])
        vs[i] = r[:, (4 + i) * HD:(5 + i) * HD].astype(BF16)
    refill(0, 560, 0, 560)

    causal = lax.broadcasted_iota(jnp.int32, (TOK, TOK), 0) >= lax.broadcasted_iota(jnp.int32, (TOK, TOK), 1)
    for i in range(HEADS):
        g = i // REP
        scores = dot_nt(qs[i], ks[g]) * (HD ** -0.5)
        weights = softmax_rows(jnp.where(causal, scores, MASK_VALUE))
        ctx[:, i * HD:(i + 1) * HD] = mm(weights, vs[g]).astype(BF16)

    def to_sib(n):
        return remote(pall.at[n, 1 - co], psib.at[n], ps_s.at[n], ps_r.at[n], sib)

    def to_cross(n, par, half):
        if half:
            rows = pl.ds(pl.multiple_of((1 - xi) * 64, 64), 64)
            return remote(csum.at[n, rows], crcv.at[par, n, rows], cs_s.at[n], cs_r.at[par, n], cross)
        return remote(csum.at[n], crcv.at[par, n], cs_s.at[n], cs_r.at[par, n], cross)

    def half_cols(n):
        return pl.ds(pl.multiple_of(n * CW + co * HW, HW), HW)

    def h_out(n):
        ref = hbuf.at[:, half_cols(n)]
        return remote(ref, ref, hh_s.at[n], hh_r.at[n], sib)

    def each(fn):
        lax.fori_loop(0, CH, lambda n, _: (fn(n), 0)[1], 0)

    def reduce_out(name, left, rows, pitch, par, half):
        first, units, _ = SEG[name]

        def pair_sum(n):
            to_sib(n).wait_recv()
            csum[n] = (pall[n, co].astype(F32) + psib[n].astype(F32)).astype(BF16)
            to_cross(n, par, half).start()

        def chunk(n):
            start = spot(name, n)
            landed(start, 4 * rows, wsem.at[SEMS[name] + n])
            part = mm(left[...], panels(start, rows, pitch, 4))
            pall[n, 0] = part[:, :HW].astype(BF16)
            pall[n, 1] = part[:, HW:].astype(BF16)
            to_sib(n).start()
            refill(first + n * units, first + (n + 1) * units, first, first + CH * units)

            @pl.when(n >= 1)
            def _():
                pair_sum(n - 1)

        each(chunk)
        pair_sum(CH - 1)

    def finish(par, factor):
        def chunk(n):
            to_cross(n, par, False).wait_recv()
            total = csum[n].astype(F32) + crcv[par, n].astype(F32)
            if factor is not None:
                total = fac[factor] * total
            cols = half_cols(n)
            hbuf[:, cols] = (hbuf[:, cols].astype(F32) + total).astype(BF16)
            h_out(n).start()

        each(chunk)

        def settle(n):
            h_out(n).wait_recv()
            h_out(n).wait_send()
            to_sib(n).wait_send()
            to_cross(n, par, False).wait_send()

        each(settle)

    def gate_up(name):
        first = SEG[name][0]

        def step(i, _):
            start = spot(name, i * 3)
            landed(start, 6 * D, wsem.at[SEMS[name] + i])
            part = mm(xn[...], panels(start, D, D, 6))
            for p in range(3):
                gate = part[:, p * 256:p * 256 + 128]
                up = part[:, p * 256 + 128:p * 256 + 256]
                act[:, pl.ds(pl.multiple_of((i * 3 + p) * 128, 128), 128)] = (jax.nn.silu(gate) * up).astype(BF16)
            refill(first + i * 240, first + (i + 1) * 240, first, first + 2160)
            return 0

        lax.fori_loop(0, 9, step, 0)

    for k in range(AGC):
        for kind in range(3):
            ag(kind, k).wait_send()
    reduce_out("o_a", ctx, 1280, 1280, 0, False)
    finish(0, None)
    for k in range(2, 5):
        vcross(k).start()
    for k in range(0, 2):
        vcross(k).wait_recv()
        vrelay(k).start()
    norm_rows(0, TOK, 1)
    gate_up("gu_a")
    reduce_out("d_a", act, FF, 30 * UNIT, 1, False)
    for k in range(5, VCH):
        vcross(k).start()

    kv_at = spot("kv_b", 0)

    def kv_block(b):
        part = mm(vbuf[b], panels(kv_at, D, D, 4))
        rows = pl.ds(pl.multiple_of(b * TOK, TOK), TOK)
        for g in range(GROUPS):
            kb[g, rows, :] = head_norm(part[:, g * HD:(g + 1) * HD], small[1:2, :]).astype(BF16)
            vb[g, rows, :] = part[:, (2 + g) * HD:(3 + g) * HD].astype(BF16)

    landed(kv_at, 4 * D, wsem.at[SEMS["kv_b"]])
    vown().wait_recv()
    lax.fori_loop(0, 2, lambda i, _: (kv_block(me + i * (sib - me)), 0)[1], 0)
    for k in range(2, 5):
        vcross(k).wait_recv()
        vrelay(k).start()
    finish(1, None)
    norm_rows(0, TOK, 2)

    at = spot("q_b", 0)
    landed(at, 8 * D, wsem.at[SEMS["q_b"]])
    r = mm(xn[...], panels(at, D, D, 8))
    for i in range(8):
        qs[i] = head_norm(r[:, i * HD:(i + 1) * HD], small[0:1, :]).astype(BF16)
    landed(at + 8 * D, 2 * D, wsem.at[SEMS["q_b"] + 1])
    r = mm(xn[...], panels(at + 8 * D, D, D, 2))
    for i in range(2):
        qs[8 + i] = head_norm(r[:, i * HD:(i + 1) * HD], small[0:1, :]).astype(BF16)
    for k in range(5, VCH):
        vcross(k).wait_recv()
        vrelay(k).start()
    for k in range(VCH):
        vrelay(k).wait_recv()
    lax.fori_loop(0, 2, lambda i, _: (kv_block(cross + i * (diag - cross)), 0)[1], 0)
    refill(4320, 4880, 4320, 4880)

    def cross_group(g, _):
        for i in range(REP):
            scores = dot_nt(qs[g * REP + i], kb[g]) * (HD ** -0.5)
            scores = jnp.concatenate(
                [jnp.where(meta[:, j + 1:j + 2] > 0.0, scores[:, j * HD:(j + 1) * HD], MASK_VALUE) for j in range(TILES)], axis=1)
            ctx[:, pl.ds(pl.multiple_of((g * REP + i) * HD, HD), HD)] = mm(softmax_rows(scores), vb[g]).astype(BF16)
        return 0

    lax.fori_loop(0, GROUPS, cross_group, 0)
    reduce_out("o_b", ctx, 1280, 1280, 0, False)
    finish(0, 0)
    norm_rows(0, TOK, 3)
    gate_up("gu_b")
    reduce_out("d_b", act, FF, 30 * UNIT, 1, True)

    chip_rows = pl.ds(pl.multiple_of(xi * 64, 64), 64)

    def fin_out(n):
        return remote(ostage.at[n, pl.ds(pl.multiple_of((1 - co) * 32, 32), 32)], fin.at[:, half_cols(n)], hh_s.at[n], hh_r.at[n], sib)

    def last(n):
        to_cross(n, 1, True).wait_recv()
        cols = half_cols(n)
        total = csum[n, chip_rows].astype(F32) + crcv[1, n, chip_rows].astype(F32)
        ostage[n] = (hbuf[chip_rows, cols].astype(F32) + fac[1, chip_rows] * total).astype(BF16)
        fin_out(n).start()
        fin[:, cols] = ostage[n, pl.ds(pl.multiple_of(co * 32, 32), 32), :]

    each(last)

    def settle(n):
        fin_out(n).wait_recv()
        fin_out(n).wait_send()
        to_sib(n).wait_send()
        to_cross(n, 1, True).wait_send()

    each(settle)
    store = pltpu.make_async_copy(fin, out.at[0], lsem.at[2])
    store.start()
    for m in metas:
        m.wait_send()
    vown().wait_send()
    for k in range(VCH):
        vcross(k).wait_send()
        vrelay(k).wait_send()
    store.wait()


def solution(mesh):
    act_spec = P('dp', 'tp', None)
    col_spec = P(None, 'tp')
    row_spec = P('tp', None)
    layer_a = (P(), col_spec, col_spec, col_spec, row_spec, P(), col_spec, col_spec, row_spec)
    layer_b = (P(), col_spec, P(), col_spec, col_spec, P(), row_spec, P(), col_spec, col_spec, row_spec, P())
    in_specs = (act_spec, act_spec, P('dp', 'tp'), act_spec) + layer_a + layer_b

    def body(hidden, vision, positions, tile_mask, ln1_a, wq_a, wk_a, wv_a, wo_a, ln2_a, wg_a, wu_a, wd_a, ln1_b, wq_b, q_norm, wk_b, wv_b, k_norm, wo_b, ln2_b, wg_b, wu_b, wd_b, xgates):
        gains = jnp.stack([ln1_a, ln2_a, ln1_b, ln2_b]).astype(F32)
        gate_vals = jnp.tanh(xgates.astype(F32))
        freq = rope_table(HD)
        ones = jnp.ones((HD,), F32)
        small = jnp.stack([q_norm.astype(F32), k_norm.astype(F32), jnp.concatenate([freq, freq]), gate_vals[0] * ones, gate_vals[1] * ones])
        vmem = pl.BlockSpec(memory_space=pltpu.VMEM)
        hbm = pl.BlockSpec(memory_space=pl.ANY)
        dma = pltpu.SemaphoreType.DMA
        return pl.pallas_call(
            kernel,
            out_shape=jax.ShapeDtypeStruct((1, 32, D), BF16),
            in_specs=[vmem] * 4 + [hbm] * 16,
            out_specs=hbm,
            scratch_shapes=[
                pltpu.VMEM((RING * UNIT, 128), BF16),
                pltpu.VMEM((TOK, D), BF16),
                pltpu.VMEM((TOK, D), BF16),
                pltpu.VMEM((4, TOK, D), BF16),
                pltpu.VMEM((TOK, 128), F32),
                pltpu.VMEM((TOK, HD), F32),
                pltpu.VMEM((TOK, HD), F32),
                pltpu.VMEM((2, TOK, HW), F32),
                pltpu.VMEM((HEADS, TOK, HD), BF16),
                pltpu.VMEM((GROUPS, TOK, HD), BF16),
                pltpu.VMEM((GROUPS, TOK, HD), BF16),
                pltpu.VMEM((GROUPS, 4 * TOK, HD), BF16),
                pltpu.VMEM((GROUPS, 4 * TOK, HD), BF16),
                pltpu.VMEM((TOK, HEADS * HD), BF16),
                pltpu.VMEM((TOK, FF), BF16),
                pltpu.VMEM((CH, 2, TOK, HW), BF16),
                pltpu.VMEM((CH, TOK, HW), BF16),
                pltpu.VMEM((CH, TOK, HW), BF16),
                pltpu.VMEM((2, CH, TOK, HW), BF16),
                pltpu.VMEM((CH, 64, HW), BF16),
                pltpu.VMEM((32, D), BF16),
                dma((NSEM,)), dma((3,)),
                dma((3, AGC)), dma((3, AGC)),
                dma((3,)), dma((3,)),
                dma((VCH,)), dma((VCH,)),
                dma((VCH,)), dma((VCH,)),
                dma(()), dma(()),
                dma((CH,)), dma((CH,)),
                dma((CH,)), dma((2, CH)),
                dma((CH,)), dma((CH,)),
            ],
            compiler_params=pltpu.CompilerParams(collective_id=0, has_side_effects=True, vmem_limit_bytes=67043328),
        )(positions, tile_mask, gains, small, hidden, vision, wq_a, wk_a, wv_a, wo_a, wg_a, wu_a, wd_a, wq_b, wk_b, wv_b, wo_b, wg_b, wu_b, wd_b)

    return jax.shard_map(body, mesh=mesh, in_specs=in_specs, out_specs=act_spec, check_vma=False)
```

```python
import math

import jax
import jax.numpy as jnp
import numpy as np
from jax import lax
from jax.experimental import pallas as pl
from jax.experimental.pallas import tpu as pltpu
from jax.sharding import PartitionSpec as P

ROPE_THETA = 500000.0
ROPE_FACTOR = 8.0
LOW_FACTOR = 1.0
HIGH_FACTOR = 4.0
ORIG_CONTEXT = 8192.0
NORM_EPS = 1e-5
MASK_VALUE = -1e30
MESH = pl.DeviceIdType.MESH
F32 = jnp.float32
BF16 = jnp.bfloat16

D = 5120
TOK = 128
HD = 128
HEADS = 10
GROUPS = 2
REP = 5
FF = 3456
TILES = 4
CH = 10
CW = D // CH
HW = CW // 2
OWN = 32
PAIR = 64
KT = 40
QW = 1280
SUB = 16
UNIT = 128
RING = 1440
AGC = 4
VCH = 16
VGROUP = (0, 5, 14, 16)
EARLY = 112

SEG = {
    "qkv_a": (0, 560, 1),
    "o_a": (560, 40, 10),
    "gu_a": (960, 80, 27),
    "d_a": (3120, 120, 10),
    "q_b": (4320, 40, 10),
    "kv_b": (4720, 160, 1),
    "o_b": (4880, 40, 10),
    "gu_b": (5280, 240, 10),
    "d_b": (7680, 120, 10),
}
SEMS = {"qkv_a": 0, "q_b": 0, "o_a": 2, "o_b": 2, "d_a": 12, "d_b": 12, "gu_a": 22, "gu_b": 22, "kv_b": 40}
NSEM = 41
GU_SEMS = 18


def rope_table(head_dim):
    low_wave = ORIG_CONTEXT / LOW_FACTOR
    high_wave = ORIG_CONTEXT / HIGH_FACTOR
    freq_list = []
    for freq_idx in range(head_dim // 2):
        base_freq = 1.0 / (ROPE_THETA ** (2.0 * freq_idx / head_dim))
        wave_len = 2.0 * math.pi / base_freq
        if wave_len > low_wave:
            freq_list.append(base_freq / ROPE_FACTOR)
        elif wave_len < high_wave:
            freq_list.append(base_freq)
        else:
            smooth = (ORIG_CONTEXT / wave_len - LOW_FACTOR) / (HIGH_FACTOR - LOW_FACTOR)
            freq_list.append((1.0 - smooth) * base_freq / ROPE_FACTOR + smooth * base_freq)
    return np.array(freq_list, dtype=np.float32)


def head_norm(values, gain):
    mean_sq = jnp.mean(values * values, axis=-1, keepdims=True)
    return values * lax.rsqrt(mean_sq + NORM_EPS) * gain


def softmax_rows(scores):
    top = jnp.max(scores, axis=-1, keepdims=True)
    weights = jnp.exp(scores - top)
    return (weights * (1.0 / jnp.sum(weights, axis=-1, keepdims=True))).astype(BF16)


def dot_nt(left, right):
    return lax.dot_general(left, right, (((1,), (1,)), ((), ())), preferred_element_type=F32)


def kernel(pos, tmask, freq, xg, ln1_a, ln2_a, ln1_b, ln2_b, qn, kn, hid, vis, wq_a, wk_a, wv_a, wo_a, wg_a, wu_a, wd_a, wq_b, wk_b, wv_b, wo_b, wg_b, wu_b, wd_b, out,
           ring, hbuf, xn, vbuf, gains, meta, cos_s, sin_s, fac, ks, vs, kb, vb, act, pall, psib, crcv, ssq, sprev, facc,
           wsem, lsem, ag_s, ag_r, mt_s, mt_r, vx_s, vx_r, vr_s, vr_r, vo_s, vo_r, ps_s, ps_r, cs_s, cs_r, hh_s, hh_r):
    me = lax.axis_index("tp")
    xi = lax.div(me, 2)
    co = lax.rem(me, 2)
    sib = xi * 2 + 1 - co
    cross = (1 - xi) * 2 + co
    diag = (1 - xi) * 2 + 1 - co

    def remote(src, dst, ssem, rsem, dev):
        return pltpu.make_async_remote_copy(src_ref=src, dst_ref=dst, send_sem=ssem, recv_sem=rsem, device_id={"tp": dev}, device_id_type=MESH)

    def spot(name, j):
        first, units, _ = SEG[name]
        return lax.rem(first + j * units, RING) * UNIT

    def panel_spot(name, j):
        return lax.rem(SEG[name][0] + j * KT, RING) * UNIT

    def put(weight, rows, col, at, sem, first=0):
        pltpu.make_async_copy(weight.at[pl.ds(first, rows), pl.ds(pl.multiple_of(col * HD, HD), HD)], ring.at[pl.ds(pl.multiple_of(at, HD), rows)], sem).start()

    def start_group(name, j):
        at = spot(name, j)
        base = SEMS[name]
        if name[:2] == "o_":
            for p in range(4):
                put(wo_a if name == "o_a" else wo_b, QW, j * 4 + p, at + p * QW, wsem.at[base + j])
        elif name == "gu_b":
            def pair(i, _):
                for p, w in enumerate((wg_b, wu_b)):
                    put(w, CW, i, at + (i * 2 + p) * CW, wsem.at[base + j], pl.multiple_of(j * CW, CW))
                return 0
            lax.fori_loop(0, FF // HD, pair, 0)
        elif name == "gu_a":
            put(wg_a, D, j, at, wsem.at[base + lax.rem(j, GU_SEMS)])
            put(wu_a, D, j, at + D, wsem.at[base + lax.rem(j, GU_SEMS)])
        elif name[:2] == "d_":
            for p in range(4):
                put(wd_a if name == "d_a" else wd_b, FF, j * 4 + p, at + p * 30 * UNIT, wsem.at[base + j])
        elif name == "q_b":
            put(wq_b, D, j, at, wsem.at[base + lax.div(j, 5)])
        elif name == "kv_b":
            for p, w in enumerate((wk_b, wk_b, wv_b, wv_b)):
                put(w, D, p % 2, at + p * D, wsem.at[base])
        else:
            for p in range(14):
                w = wq_a if p < 10 else (wk_a if p < 12 else wv_a)
                put(w, D, p if p < 10 else p % 2, at + p * D, wsem.at[base + p // 8])

    def ready(name, freed):
        first, units, count = SEG[name]
        if isinstance(freed, int):
            return min(max((freed + RING - first) // units, 0), count)
        return jnp.minimum(jnp.maximum(lax.div(freed + RING - first + 100 * units, units) - 100, 0), count)

    def refill(before, after, low, high, names=tuple(SEG)):
        for name in names:
            first, units, count = SEG[name]
            if first + units > high + RING or first + units * count <= low + RING:
                continue
            lo, hi = ready(name, before), ready(name, after)
            if isinstance(lo, int) and isinstance(hi, int) and lo >= hi:
                continue
            lax.fori_loop(lo, hi, lambda j, _, name=name: (start_group(name, j), 0)[1], 0)

    def landed(at, rows, sem):
        span = ring.at[pl.ds(pl.multiple_of(at, HD), rows)]
        pltpu.make_async_copy(span, span, sem).wait()

    def panel_set(spots, rows):
        return jnp.concatenate([ring[pl.ds(pl.multiple_of(at, HD), rows), :] for at in spots], axis=1)

    def panels(at, rows, pitch, count):
        return jnp.concatenate([ring[pl.ds(pl.multiple_of(at + p * pitch, HD), rows), :] for p in range(count)], axis=1)

    def mm(left, right):
        return jnp.dot(left, right, preferred_element_type=F32)

    def q_cols(i):
        start = (HEADS + i) * HD
        return pl.ds(start if isinstance(i, int) else pl.multiple_of(start, HD), HD)

    def q_group(g):
        return jnp.concatenate([act[:, q_cols(g * REP + i)] for i in range(REP)], axis=0)

    own_rows = pl.ds(pl.multiple_of(me * OWN, OWN), OWN)
    load_h = pltpu.make_async_copy(hid.at[0], hbuf.at[own_rows], lsem.at[0])
    load_h.start()
    load_v = pltpu.make_async_copy(vis.at[0], vbuf.at[me], lsem.at[1])
    load_v.start()
    barrier = pltpu.get_barrier_semaphore()
    for dev in (sib, cross, diag):
        pl.semaphore_signal(barrier, inc=1, device_id={"tp": dev}, device_id_type=MESH)
    for name in SEG:
        for j in range(ready(name, 0) if name == "qkv_a" else 0):
            start_group(name, j)
    row_i = lax.broadcasted_iota(jnp.int32, (OWN, HD), 0)
    lane_i = lax.broadcasted_iota(jnp.int32, (OWN, HD), 1)
    pos_row = jnp.concatenate([jnp.broadcast_to(pos[...].astype(F32), (OWN, OWN)), jnp.zeros((OWN, 96), F32)], axis=1)
    pos_col = jnp.sum(jnp.where(row_i == lane_i, pos_row, 0.0), axis=1, keepdims=True)
    own_meta = jnp.where(lane_i == 0, pos_col, 0.0)
    for j in range(TILES):
        tm_row = jnp.concatenate([jnp.broadcast_to(tmask[0, j:j + 1, :].astype(F32), (OWN, OWN)), jnp.zeros((OWN, 96), F32)], axis=1)
        tm_col = jnp.sum(jnp.where(row_i == lane_i, tm_row, 0.0), axis=1, keepdims=True)
        own_meta = jnp.where(lane_i == j + 1, tm_col, own_meta)
    meta[own_rows, :] = own_meta
    load_h.wait()
    pl.semaphore_wait(barrier, 3)

    def ag(kind, k):
        cols = pl.ds(k * (D // AGC), D // AGC)
        rows = pl.ds(pl.multiple_of((cross if kind == 2 else me) * OWN, OWN), OWN)
        ref = hbuf.at[rows, cols]
        return remote(ref, ref, ag_s, ag_r.at[(4, k, 5)[kind]], cross if kind == 1 else sib)

    def vown():
        return remote(vbuf.at[me], vbuf.at[me], vo_s, vo_r, sib)

    def vpiece(owner, k):
        return vbuf.at[owner, pl.ds(k // 2 * SUB, SUB), pl.ds(k % 2 * (D // 2), D // 2)]

    def vgroup(k):
        return 0 if k < VGROUP[1] else (1 if k < VGROUP[2] else 2)

    def vcross(k):
        return remote(vpiece(me, k), vpiece(me, k), vx_s, vx_r.at[vgroup(k)], cross)

    def vrelay(k):
        return remote(vpiece(cross, k), vpiece(cross, k), vr_s, vr_r.at[vgroup(k)], sib)

    def relay_vision(g):
        landed(0, (VGROUP[g + 1] - VGROUP[g]) * 320, vx_r.at[g])
        for k in range(VGROUP[g], VGROUP[g + 1]):
            vrelay(k).start()

    for k in range(AGC):
        ag(0, k).start()
    for k in range(AGC):
        ag(1, k).start()
    metas = [remote(meta.at[own_rows], meta.at[own_rows], mt_s, mt_r, dev) for dev in (sib, cross, diag)]
    for m in metas:
        m.start()
    load_v.wait()
    for k in range(5):
        vcross(k).start()

    for i, ln in enumerate((ln1_a, ln2_a, ln1_b, ln2_b)):
        for p in range(D // HD):
            gains[i:i + 1, p * HD:(p + 1) * HD] = ln[p:p + 1, :].astype(F32)
    q_gain = qn[...].astype(F32)
    k_gain = kn[...].astype(F32)

    def norm_rows(first, count, gain):
        def block(b, _):
            rows = pl.ds(pl.multiple_of(first + b * SUB, SUB), SUB)
            v = hbuf[rows, :].astype(F32)
            scale = lax.rsqrt(jnp.mean(v * v, axis=-1, keepdims=True) + NORM_EPS)
            xn[rows, :] = (v * scale * gains[gain:gain + 1, :]).astype(BF16)
            return 0
        lax.fori_loop(0, count // SUB, block, 0)

    norm_rows(me * OWN, OWN, 0)
    landed(0, OWN * KT, ag_r.at[4])
    norm_rows(sib * OWN, OWN, 0)
    landed(0, 3 * PAIR, mt_r)
    angles = meta[:, 0:1] * freq[...]
    cos_s[...] = jnp.cos(angles)
    lanes = lax.broadcasted_iota(jnp.int32, (TOK, HD), 1)
    sin_s[...] = jnp.where(lanes < HD // 2, -jnp.sin(angles), jnp.sin(angles))
    keep = jnp.max(jnp.where((lanes >= 1) & (lanes <= TILES), meta[...], 0.0), axis=1, keepdims=True)
    for i in range(2):
        fac[i] = jnp.where(keep > 0.0, jnp.tanh(jnp.full((TOK, HW), xg[i], F32)), 0.0)
    for k in range(AGC):
        ag(1, k).wait_recv()
        ag(2, k).start()
    refill(-RING, 0, 560 - RING, 0)
    norm_rows(cross * OWN, OWN, 0)

    landed(0, OWN * KT, ag_r.at[5])
    norm_rows(diag * OWN, OWN, 0)
    vown().start()

    def rope(v):
        return (v * cos_s[...] + pltpu.roll(v, HD // 2, 1) * sin_s[...]).astype(BF16)

    at = spot("qkv_a", 0)
    landed(at, 8 * D, wsem.at[0])
    landed(at + 8 * D, 6 * D, wsem.at[1])
    r = mm(xn[...], panels(at, D, D, 8))
    for i in range(8):
        act[:, q_cols(i)] = rope(r[:, i * HD:(i + 1) * HD])
    r = mm(xn[...], panels(at + 8 * D, D, D, 6))
    for i in range(2):
        act[:, q_cols(8 + i)] = rope(r[:, i * HD:(i + 1) * HD])
        ks[i] = rope(r[:, (2 + i) * HD:(3 + i) * HD])
        vs[i] = r[:, (4 + i) * HD:(5 + i) * HD].astype(BF16)
    refill(0, 560, 0, 560)

    causal = lax.rem(lax.broadcasted_iota(jnp.int32, (REP * TOK, TOK), 0), TOK) >= lax.broadcasted_iota(jnp.int32, (REP * TOK, TOK), 1)
    for g in range(GROUPS):
        scores = dot_nt(q_group(g), ks[g]) * (HD ** -0.5)
        mixed = mm(softmax_rows(jnp.where(causal, scores, MASK_VALUE)), vs[g]).astype(BF16)
        for i in range(REP):
            act[:, (g * REP + i) * HD:(g * REP + i + 1) * HD] = mixed[i * TOK:(i + 1) * TOK]

    def to_sib(n):
        return remote(pall.at[n, 1 - co], psib.at[n], ps_s, ps_r.at[n], sib)

    def to_cross(n, par, half):
        if half:
            rows = pl.ds(pl.multiple_of((1 - xi) * PAIR, PAIR), PAIR)
            return remote(pall.at[n, co, rows], crcv.at[par, n, rows], cs_s, cs_r.at[par, n], cross)
        return remote(pall.at[n, co], crcv.at[par, n], cs_s, cs_r.at[par, n], cross)

    def half_cols(n):
        return pl.ds(pl.multiple_of(n * CW + co * HW, HW), HW)

    def h_out(n):
        ref = hbuf.at[:, half_cols(n)]
        return remote(ref, ref, hh_s, hh_r.at[n], sib)

    def each(fn):
        lax.fori_loop(0, CH, lambda n, _: (fn(n), 0)[1], 0)

    def reduce_out(name, left, rows, pitch, par, half, early, lag, fill=None):
        first, units, _ = SEG[name]

        def pair_sum(n):
            to_sib(n).wait_recv()
            pall[n, co] = (pall[n, co].astype(F32) + psib[n].astype(F32)).astype(BF16)
            to_cross(n, par, half).start()

        def chunk(n):
            start = spot(name, n)
            landed(start, 4 * rows, wsem.at[SEMS[name] + n])
            part = mm(left[...], panels(start, rows, pitch, 4))
            part = part.astype(BF16)
            for k in range(2):
                if half:
                    blocks = [part[r:r + OWN, q:q + HW] for r in (OWN * k, PAIR + OWN * k) for q in (0, HW)]
                    pall[n, k] = jnp.concatenate(blocks, axis=0)
                else:
                    pall[n, k] = part[:, k * HW:(k + 1) * HW]
            to_sib(n).start()
            if fill is None:
                refill(first + n * units, first + (n + 1) * units, first, first + CH * units)
            else:
                fill(n)

            if early < lag:
                @pl.when(n == early)
                def _():
                    pair_sum(0)

            @pl.when(n >= (lag if early == lag else lag + 1))
            def _():
                pair_sum(n - lag)

        each(chunk)
        for n in range(CH - lag, CH):
            pair_sum(n)

    def finish(par, factor, gain):
        def squares(v):
            v = v.astype(F32)
            v = v * v
            ssq[...] += v[:, :HD] + v[:, HD:]

        def absorb(n):
            h_out(n).wait_recv()
            squares(hbuf[:, pl.ds(pl.multiple_of(n * CW + (1 - co) * HW, HW), HW)])

        def chunk(n):
            to_cross(n, par, False).wait_recv()
            total = pall[n, co].astype(F32) + crcv[par, n].astype(F32)
            if factor is not None:
                total = fac[factor] * total
            cols = half_cols(n)
            fresh = (hbuf[:, cols].astype(F32) + total).astype(BF16)
            hbuf[:, cols] = fresh
            h_out(n).start()
            squares(fresh)

            @pl.when(n >= 2)
            def _():
                absorb(n - 2)

        ssq[...] = jnp.zeros_like(ssq)
        each(chunk)
        absorb(CH - 2)
        absorb(CH - 1)
        ssq[...] = jnp.broadcast_to(lax.rsqrt(jnp.sum(ssq[...], axis=1, keepdims=True) * (1.0 / D) + NORM_EPS), (TOK, HD))

        def block(b, _):
            rows = pl.ds(pl.multiple_of(b * SUB, SUB), SUB)
            xn[rows, :] = (hbuf[rows, :].astype(F32) * ssq[rows, 0:1] * gains[gain:gain + 1, :]).astype(BF16)
            return 0

        lax.fori_loop(0, TOK // SUB, block, 0)

        for sem in (hh_s, ps_s, cs_s):
            landed(0, CH * 2 * TOK, sem)

    def gate_up(name):
        first = SEG[name][0]

        def pairs(j, count):
            spots = [panel_spot(name, j * 2 + p) for p in range(2 * count)]
            for p in range(count):
                landed(spots[p * 2], 2 * D, wsem.at[SEMS[name] + lax.rem(j + p, GU_SEMS)])
            part = mm(xn[...], panel_set(spots, D))
            for p in range(count):
                gate = part[:, p * HW:p * HW + HD]
                up = part[:, p * HW + HD:p * HW + HW]
                act[:, pl.ds(pl.multiple_of((j + p) * HD, HD), HD)] = (jax.nn.silu(gate) * up).astype(BF16)
            refill(first + j * 80, first + (j + count) * 80, first, first + 2160, ("gu_a", "d_a"))

        lax.fori_loop(0, 6, lambda i, _: (pairs(i * 4, 4), 0)[1], 0)
        pairs(jnp.int32(24), 3)

    landed(0, 3 * OWN * KT, ag_s)
    reduce_out("o_a", act.at[:, 0:HEADS * HD], QW, QW, 0, False, 2, 2)
    for k in range(5, 14):
        vcross(k).start()
    finish(0, None, 1)
    relay_vision(0)
    gate_up("gu_a")

    def fill_late(n):
        @pl.when(n == CH // 2)
        def _():
            refill(0, 3840, 0, 3840, ("q_b", "kv_b"))

    reduce_out("d_a", act, FF, 30 * UNIT, 1, False, 1, 2, fill_late)
    for k in range(14, VCH):
        vcross(k).start()

    kv_at = spot("kv_b", 0)

    def kv_rows(states, spots):
        part = mm(states, panels(kv_at, D, D, 4))
        done = 0
        for rows, count in spots:
            piece = part[done:done + count]
            for g in range(GROUPS):
                kb[g, rows, :] = head_norm(piece[:, g * HD:(g + 1) * HD], k_gain).astype(BF16)
                vb[g, rows, :] = piece[:, (2 + g) * HD:(3 + g) * HD].astype(BF16)
            done += count

    def block_rows(b, start, count):
        return pl.ds(pl.multiple_of(b * TOK + start, SUB), count)

    landed(kv_at, 4 * D, wsem.at[SEMS["kv_b"]])
    vown().wait_recv()

    def near(i, _):
        b = me + i * (sib - me)
        kv_rows(vbuf[b], [(block_rows(b, 0, TOK), TOK)])
        return 0

    def far(i, _):
        b = cross + i * (diag - cross)
        kv_rows(vbuf[b, 0:EARLY, :], [(block_rows(b, 0, EARLY), EARLY)])
        return 0

    lax.fori_loop(0, 2, near, 0)
    relay_vision(1)
    refill(0, 4320, 0, 4320, ("o_b", "gu_b"))
    for g in range(2):
        landed(0, (VGROUP[g + 1] - VGROUP[g]) * 320, vr_r.at[g])
    lax.fori_loop(0, 2, far, 0)
    finish(1, None, 2)
    sprev[...] = ssq[...]

    q_spots = [panel_spot("q_b", j) for j in range(HEADS)]
    for i in range(2):
        landed(q_spots[i * 5], 5 * D, wsem.at[SEMS["q_b"] + i])
    for g in range(GROUPS):
        if g == 1:
            relay_vision(2)
        r = mm(xn[...], panel_set(q_spots[g * REP:(g + 1) * REP], D))
        for i in range(REP):
            act[:, q_cols(g * REP + i)] = head_norm(r[:, i * HD:(i + 1) * HD], q_gain).astype(BF16)
    refill(4320, 4720, 4320, 4720)
    landed(0, (VGROUP[3] - VGROUP[2]) * 320, vr_r.at[2])
    rest = TOK - EARLY
    kv_rows(jnp.concatenate([vbuf[cross, EARLY:, :], vbuf[diag, EARLY:, :]], axis=0),
            [(block_rows(b, EARLY, rest), rest) for b in (cross, diag)])
    refill(4720, 4880, 4720, 4880)

    for i in range(HEADS):
        scores = dot_nt(act[:, q_cols(i)], kb[i // REP]) * (HD ** -0.5)
        facc[2 * i] = scores[:, :HW]
        facc[2 * i + 1] = scores[:, HW:]

    def soft(b, _):
        rows = pl.ds(pl.multiple_of(b * OWN, OWN), OWN)
        seen = [jnp.broadcast_to(meta[rows, j + 1:j + 2], (OWN, HD)) > 0.0 for j in range(TILES)]
        for i in range(HEADS):
            parts = [facc[2 * i + j // 2, rows, j % 2 * HD:(j % 2 + 1) * HD] for j in range(TILES)]
            weights = softmax_rows(jnp.concatenate([jnp.where(m, v, MASK_VALUE) for m, v in zip(seen, parts)], axis=1))
            pall[i, 0, rows] = weights[:, :HW]
            pall[i, 1, rows] = weights[:, HW:]
        return 0

    lax.fori_loop(0, TOK // OWN, soft, 0)
    for g in range(GROUPS):
        heads = range(g * REP, (g + 1) * REP)
        mixed = sum(mm(jnp.concatenate([pall[i, p] for i in heads], axis=0), vb[g, p * HW:(p + 1) * HW, :]) for p in range(2)).astype(BF16)
        for n, i in enumerate(heads):
            act[:, i * HD:(i + 1) * HD] = mixed[n * TOK:(n + 1) * TOK]

    reduce_out("o_b", act.at[:, 0:HEADS * HD], QW, QW, 0, False, 2, 3)
    def finish_gate_up():
        first = SEG["gu_b"][0]

        def take(v, cols):
            v = v.astype(F32)
            sq = v * v
            ssq[...] += sq[:, :HD] + sq[:, HD:]
            xn[:, cols] = (v * sprev[:, 0:1] * gains[3:4, cols]).astype(BF16)

        def absorb(n):
            h_out(n).wait_recv()
            cols = pl.ds(pl.multiple_of(n * CW + (1 - co) * HW, HW), HW)
            take(hbuf[:, cols], cols)

        def own(n):
            to_cross(n, 0, False).wait_recv()
            cols = half_cols(n)
            total = fac[0] * (pall[n, co].astype(F32) + crcv[0, n].astype(F32))
            fresh = (hbuf[:, cols].astype(F32) + total).astype(BF16)
            hbuf[:, cols] = fresh
            h_out(n).start()
            take(fresh, cols)

        def products(n, store):
            at = spot("gu_b", n)
            left = xn[:, pl.ds(pl.multiple_of(n * CW, CW), CW)]
            for p in range(0, FF // HD, 4):
                count = min(4, FF // HD - p)
                part = mm(left, panel_set([at + (p * 2 + j) * CW for j in range(2 * count)], CW))
                for q in range(count):
                    store(p + q, part[:, q * HW:(q + 1) * HW])

        def arrive(n):
            landed(spot("gu_b", n), FF // PAIR * CW, wsem.at[SEMS["gu_b"] + n])

        def add(p, part):
            facc[p] += part

        def middle(n):
            absorb(n)
            arrive(n)
            products(n, add)

            refill(first + n * 240, first + (n + 1) * 240, first, first + 2160)

        def step(n):
            own(n)

            @pl.when(n >= 1)
            def _():
                middle(n - 1)

        ssq[...] = jnp.zeros_like(ssq)
        facc[...] = jnp.zeros_like(facc)
        each(step)
        last_n = jnp.int32(CH - 1)
        absorb(last_n)
        arrive(last_n)
        scale = lax.rsqrt(jnp.sum(ssq[...], axis=1, keepdims=True) * (1.0 / D) + NORM_EPS)
        ssq[...] = jnp.broadcast_to(scale, (TOK, HD)) / sprev[...]

        def activate(p, part):
            both = facc[p] + part
            act[:, p * HD:(p + 1) * HD] = (jax.nn.silu(both[:, :HD] * ssq[...]) * (both[:, HD:] * ssq[...])).astype(BF16)

        products(last_n, activate)
        refill(first + 2160, first + 2400, first + 2160, first + 2400)

        for sem in (hh_s, ps_s, cs_s):
            landed(0, CH * 2 * TOK, sem)

    finish_gate_up()
    vown().wait_send()
    landed(0, TOK * KT, vx_s)
    landed(0, TOK * KT, vr_s)
    reduce_out("d_b", act, FF, 30 * UNIT, 1, True, 2, 2)

    chip_rows = pl.ds(pl.multiple_of(xi * PAIR, PAIR), PAIR)

    def last(n):
        to_cross(n, 1, True).wait_recv()
        total = pall[n, co, chip_rows].astype(F32) + crcv[1, n, chip_rows].astype(F32)
        for q in range(2):
            cols = pl.ds(pl.multiple_of(n * CW + q * HW, HW), HW)
            xn[0:OWN, cols] = (hbuf[own_rows, cols].astype(F32) + fac[1, own_rows] * total[q * OWN:(q + 1) * OWN]).astype(BF16)
        cols = pl.ds(pl.multiple_of(n * CW, CW), CW)
        pltpu.make_async_copy(xn.at[0:OWN, cols], out.at[0, :, cols], lsem.at[2]).start()

    each(last)
    landed(0, CH * 2 * TOK, ps_s)
    landed(0, CH * TOK, cs_s)
    landed(0, 3 * PAIR, mt_s)
    landed(0, OWN * KT, lsem.at[2])


def solution(mesh):
    act_spec = P('dp', 'tp', None)
    col_spec = P(None, 'tp')
    row_spec = P('tp', None)
    layer_a = (P(), col_spec, col_spec, col_spec, row_spec, P(), col_spec, col_spec, row_spec)
    layer_b = (P(), col_spec, P(), col_spec, col_spec, P(), row_spec, P(), col_spec, col_spec, row_spec, P())
    in_specs = (act_spec, act_spec, P('dp', 'tp'), act_spec) + layer_a + layer_b

    def body(hidden, vision, positions, tile_mask, ln1_a, wq_a, wk_a, wv_a, wo_a, ln2_a, wg_a, wu_a, wd_a, ln1_b, wq_b, q_norm, wk_b, wv_b, k_norm, wo_b, ln2_b, wg_b, wu_b, wd_b, xgates):
        freq = rope_table(HD)
        freq = jnp.asarray(np.concatenate([freq, freq])[None, :])
        lns = [g.reshape(D // HD, HD) for g in (ln1_a, ln2_a, ln1_b, ln2_b)]
        heads = [g.reshape(1, HD) for g in (q_norm, k_norm)]
        vmem = pl.BlockSpec(memory_space=pltpu.VMEM)
        hbm = pl.BlockSpec(memory_space=pl.ANY)
        dma = pltpu.SemaphoreType.DMA
        return pl.pallas_call(
            kernel,
            out_shape=jax.ShapeDtypeStruct((1, OWN, D), BF16),
            in_specs=[vmem] * 3 + [pl.BlockSpec(memory_space=pltpu.SMEM)] + [vmem] * 6 + [hbm] * SUB,
            out_specs=hbm,
            scratch_shapes=[
                pltpu.VMEM((RING * UNIT, HD), BF16),
                pltpu.VMEM((TOK, D), BF16),
                pltpu.VMEM((TOK, D), BF16),
                pltpu.VMEM((4, TOK, D), BF16),
                pltpu.VMEM((4, D), F32),
                pltpu.VMEM((TOK, HD), F32),
                pltpu.VMEM((TOK, HD), F32),
                pltpu.VMEM((TOK, HD), F32),
                pltpu.VMEM((2, TOK, HW), F32),
                pltpu.VMEM((GROUPS, TOK, HD), BF16),
                pltpu.VMEM((GROUPS, TOK, HD), BF16),
                pltpu.VMEM((GROUPS, 4 * TOK, HD), BF16),
                pltpu.VMEM((GROUPS, 4 * TOK, HD), BF16),
                pltpu.VMEM((TOK, FF), BF16),
                pltpu.VMEM((CH, 2, TOK, HW), BF16),
                pltpu.VMEM((CH, TOK, HW), BF16),
                pltpu.VMEM((2, CH, TOK, HW), BF16),
                pltpu.VMEM((TOK, HD), F32),
                pltpu.VMEM((TOK, HD), F32),
                pltpu.VMEM((FF // HD, TOK, HW), F32),
                dma((NSEM,)), dma((3,)),
                dma(()), dma((6,)),
                dma(()), dma(()),
                dma(()), dma((3,)),
                dma(()), dma((3,)),
                dma(()), dma(()),
                dma(()), dma((CH,)),
                dma(()), dma((2, CH)),
                dma(()), dma((CH,)),
            ],
            compiler_params=pltpu.CompilerParams(collective_id=0, has_side_effects=True, vmem_limit_bytes=67043328),
        )(positions, jnp.swapaxes(tile_mask, 1, 2), freq, xgates, *lns, *heads, hidden, vision, wq_a, wk_a, wv_a, wo_a, wg_a, wu_a, wd_a, wq_b, wk_b, wv_b, wo_b, wg_b, wu_b, wd_b)

    return jax.shard_map(body, mesh=mesh, in_specs=in_specs, out_specs=act_spec, check_vma=False)
```

```python
import math

import jax
import jax.numpy as jnp
import numpy as np
from jax import lax
from jax.experimental import pallas as pl
from jax.experimental.pallas import tpu as pltpu
from jax.sharding import PartitionSpec as P

ROPE_THETA = 500000.0
ROPE_FACTOR = 8.0
LOW_FACTOR = 1.0
HIGH_FACTOR = 4.0
ORIG_CONTEXT = 8192.0
NORM_EPS = 1e-5
MASK_VALUE = -1e30
MESH = pl.DeviceIdType.MESH
F32 = jnp.float32
BF16 = jnp.bfloat16

D = 5120
TOK = 128
HD = 128
HEADS = 10
GROUPS = 2
REP = 5
FF = 3456
TILES = 4
CH = 10
CW = D // CH
HW = CW // 2
OWN = 32
PAIR = 64
KT = 40
QW = 1280
SUB = 16
UNIT = 128
RING = 1440
AGC = 4
VCH = 16
VGROUP = (0, 5, 14, 16)
EARLY = 112

SEG = {
    "qkv_a": (0, 560, 1),
    "o_a": (560, 40, 10),
    "gu_a": (960, 80, 27),
    "d_a": (3120, 120, 10),
    "q_b": (4320, 40, 10),
    "kv_b": (4720, 160, 1),
    "o_b": (4880, 40, 10),
    "gu_b": (5280, 240, 10),
    "d_b": (7680, 120, 10),
}
SEMS = {"qkv_a": 0, "q_b": 0, "o_a": 2, "o_b": 2, "d_a": 12, "d_b": 12, "gu_a": 22, "gu_b": 22, "kv_b": 40}
NSEM = 41
GU_SEMS = 18


def rope_table(head_dim):
    low_wave = ORIG_CONTEXT / LOW_FACTOR
    high_wave = ORIG_CONTEXT / HIGH_FACTOR
    freq_list = []
    for freq_idx in range(head_dim // 2):
        base_freq = 1.0 / (ROPE_THETA ** (2.0 * freq_idx / head_dim))
        wave_len = 2.0 * math.pi / base_freq
        if wave_len > low_wave:
            freq_list.append(base_freq / ROPE_FACTOR)
        elif wave_len < high_wave:
            freq_list.append(base_freq)
        else:
            smooth = (ORIG_CONTEXT / wave_len - LOW_FACTOR) / (HIGH_FACTOR - LOW_FACTOR)
            freq_list.append((1.0 - smooth) * base_freq / ROPE_FACTOR + smooth * base_freq)
    return np.array(freq_list, dtype=np.float32)


def head_norm(values, gain):
    mean_sq = jnp.mean(values * values, axis=-1, keepdims=True)
    return values * lax.rsqrt(mean_sq + NORM_EPS) * gain


def softmax_rows(scores):
    top = jnp.max(scores, axis=-1, keepdims=True)
    weights = jnp.exp(scores - top)
    return (weights * (1.0 / jnp.sum(weights, axis=-1, keepdims=True))).astype(BF16)


def dot_nt(left, right):
    return lax.dot_general(left, right, (((1,), (1,)), ((), ())), preferred_element_type=F32)


def kernel(pos, tmask, freq, xg, ln1_a, ln2_a, ln1_b, ln2_b, qn, kn, hid, vis, wq_a, wk_a, wv_a, wo_a, wg_a, wu_a, wd_a, wq_b, wk_b, wv_b, wo_b, wg_b, wu_b, wd_b, out,
           ring, hbuf, xn, vbuf, gains, meta, cos_s, sin_s, fac, ks, vs, kb, vb, act, pall, psib, crcv, ssq, sprev, facc,
           wsem, lsem, ag_s, ag_r, mt_s, mt_r, vx_s, vx_r, vr_s, vr_r, vo_s, vo_r, ps_s, ps_r, cs_s, cs_r, hh_s, hh_r):
    me = lax.axis_index("tp")
    xi = lax.div(me, 2)
    co = lax.rem(me, 2)
    sib = xi * 2 + 1 - co
    cross = (1 - xi) * 2 + co
    diag = (1 - xi) * 2 + 1 - co

    def remote(src, dst, ssem, rsem, dev):
        return pltpu.make_async_remote_copy(src_ref=src, dst_ref=dst, send_sem=ssem, recv_sem=rsem, device_id={"tp": dev}, device_id_type=MESH)

    def spot(name, j):
        first, units, _ = SEG[name]
        return lax.rem(first + j * units, RING) * UNIT

    def panel_spot(name, j):
        return lax.rem(SEG[name][0] + j * KT, RING) * UNIT

    def put(weight, rows, col, at, sem, first=0):
        pltpu.make_async_copy(weight.at[pl.ds(first, rows), pl.ds(pl.multiple_of(col * HD, HD), HD)], ring.at[pl.ds(pl.multiple_of(at, HD), rows)], sem).start()

    def start_group(name, j):
        at = spot(name, j)
        base = SEMS[name]
        if name[:2] == "o_":
            for p in range(4):
                put(wo_a if name == "o_a" else wo_b, QW, j * 4 + p, at + p * QW, wsem.at[base + j])
        elif name == "gu_b":
            def pairs(i, _):
                for q in range(9):
                    for p, w in enumerate((wg_b, wu_b)):
                        put(w, CW, i * 9 + q, at + (i * 18 + q * 2 + p) * CW, wsem.at[base + j], pl.multiple_of(j * CW, CW))
                return 0
            lax.fori_loop(0, FF // HD // 9, pairs, 0)
        elif name == "gu_a":
            put(wg_a, D, j, at, wsem.at[base + lax.rem(j, GU_SEMS)])
            put(wu_a, D, j, at + D, wsem.at[base + lax.rem(j, GU_SEMS)])
        elif name[:2] == "d_":
            for p in range(4):
                put(wd_a if name == "d_a" else wd_b, FF, j * 4 + p, at + p * 30 * UNIT, wsem.at[base + j])
        elif name == "q_b":
            put(wq_b, D, j, at, wsem.at[base + lax.div(j, 5)])
        elif name == "kv_b":
            for p, w in enumerate((wk_b, wk_b, wv_b, wv_b)):
                put(w, D, p % 2, at + p * D, wsem.at[base])
        else:
            for p in range(14):
                w = wq_a if p < 10 else (wk_a if p < 12 else wv_a)
                put(w, D, p if p < 10 else p % 2, at + p * D, wsem.at[base + p // 8])

    def ready(name, freed):
        first, units, count = SEG[name]
        if isinstance(freed, int):
            return min(max((freed + RING - first) // units, 0), count)
        return jnp.minimum(jnp.maximum(lax.div(freed + RING - first + 100 * units, units) - 100, 0), count)

    def refill(before, after, low, high, names=tuple(SEG)):
        for name in names:
            first, units, count = SEG[name]
            if first + units > high + RING or first + units * count <= low + RING:
                continue
            lo, hi = ready(name, before), ready(name, after)
            if isinstance(lo, int) and isinstance(hi, int) and lo >= hi:
                continue
            lax.fori_loop(lo, hi, lambda j, _, name=name: (start_group(name, j), 0)[1], 0)

    def start_all(name):
        lax.fori_loop(0, SEG[name][2], lambda j, _: (start_group(name, j), 0)[1], 0)

    def landed(at, rows, sem):
        span = ring.at[pl.ds(pl.multiple_of(at, HD), rows)]
        pltpu.make_async_copy(span, span, sem).wait()

    def panel_set(spots, rows):
        return jnp.concatenate([ring[pl.ds(pl.multiple_of(at, HD), rows), :] for at in spots], axis=1)

    def panels(at, rows, pitch, count):
        return jnp.concatenate([ring[pl.ds(pl.multiple_of(at + p * pitch, HD), rows), :] for p in range(count)], axis=1)

    def mm(left, right):
        return jnp.dot(left, right, preferred_element_type=F32)

    def q_cols(i):
        start = (HEADS + i) * HD
        return pl.ds(start if isinstance(i, int) else pl.multiple_of(start, HD), HD)

    def q_group(g):
        return jnp.concatenate([act[:, q_cols(g * REP + i)] for i in range(REP)], axis=0)

    own_rows = pl.ds(pl.multiple_of(me * OWN, OWN), OWN)
    load_h = pltpu.make_async_copy(hid.at[0], hbuf.at[own_rows], lsem.at[0])
    load_h.start()
    load_v = pltpu.make_async_copy(vis.at[0], vbuf.at[me], lsem.at[1])
    barrier = pltpu.get_barrier_semaphore()
    for dev in (sib, cross, diag):
        pl.semaphore_signal(barrier, inc=1, device_id={"tp": dev}, device_id_type=MESH)
    row_i = lax.broadcasted_iota(jnp.int32, (OWN, HD), 0)
    lane_i = lax.broadcasted_iota(jnp.int32, (OWN, HD), 1)
    pos_row = jnp.concatenate([jnp.broadcast_to(pos[...].astype(F32), (OWN, OWN)), jnp.zeros((OWN, 96), F32)], axis=1)
    pos_col = jnp.sum(jnp.where(row_i == lane_i, pos_row, 0.0), axis=1, keepdims=True)
    own_meta = jnp.where(lane_i == 0, pos_col, 0.0)
    for j in range(TILES):
        tm_row = jnp.concatenate([jnp.broadcast_to(tmask[0, j:j + 1, :].astype(F32), (OWN, OWN)), jnp.zeros((OWN, 96), F32)], axis=1)
        tm_col = jnp.sum(jnp.where(row_i == lane_i, tm_row, 0.0), axis=1, keepdims=True)
        own_meta = jnp.where(lane_i == j + 1, tm_col, own_meta)
    meta[own_rows, :] = own_meta
    load_h.wait()
    pl.semaphore_wait(barrier, 3)

    def ag(kind, k):
        cols = pl.ds(k * (D // AGC), D // AGC)
        rows = pl.ds(pl.multiple_of((cross if kind == 2 else me) * OWN, OWN), OWN)
        ref = hbuf.at[rows, cols]
        return remote(ref, ref, ag_s, ag_r.at[(4, k, 5)[kind]], cross if kind == 1 else sib)

    def vown():
        return remote(vbuf.at[me], vbuf.at[me], vo_s, vo_r, sib)

    def vpiece(owner, k):
        return vbuf.at[owner, pl.ds(k // 2 * SUB, SUB), pl.ds(k % 2 * (D // 2), D // 2)]

    def vgroup(k):
        return 0 if k < VGROUP[1] else (1 if k < VGROUP[2] else 2)

    def vcross(k):
        return remote(vpiece(me, k), vpiece(me, k), vx_s, vx_r.at[vgroup(k)], cross)

    def vrelay(k):
        return remote(vpiece(cross, k), vpiece(cross, k), vr_s, vr_r.at[vgroup(k)], sib)

    def relay_vision(g):
        landed(0, (VGROUP[g + 1] - VGROUP[g]) * 320, vx_r.at[g])
        for k in range(VGROUP[g], VGROUP[g + 1]):
            vrelay(k).start()

    for k in range(AGC):
        ag(0, k).start()
    for k in range(AGC):
        ag(1, k).start()
    metas = [remote(meta.at[own_rows], meta.at[own_rows], mt_s, mt_r, dev) for dev in (sib, cross, diag)]
    for m in metas:
        m.start()
    load_v.start()
    start_group("qkv_a", 0)

    for i, ln in enumerate((ln1_a, ln2_a, ln1_b, ln2_b)):
        for p in range(D // HD):
            gains[i:i + 1, p * HD:(p + 1) * HD] = ln[p:p + 1, :].astype(F32)
    q_gain = qn[...].astype(F32)
    k_gain = kn[...].astype(F32)

    def norm_rows(first, count, gain):
        def block(b, _):
            rows = pl.ds(pl.multiple_of(first + b * SUB, SUB), SUB)
            v = hbuf[rows, :].astype(F32)
            scale = lax.rsqrt(jnp.mean(v * v, axis=-1, keepdims=True) + NORM_EPS)
            xn[rows, :] = (v * scale * gains[gain:gain + 1, :]).astype(BF16)
            return 0
        lax.fori_loop(0, count // SUB, block, 0)

    norm_rows(me * OWN, OWN, 0)
    landed(0, OWN * KT, ag_r.at[4])
    norm_rows(sib * OWN, OWN, 0)
    landed(0, 3 * PAIR, mt_r)
    angles = meta[:, 0:1] * freq[...]
    cos_s[...] = jnp.cos(angles)
    lanes = lax.broadcasted_iota(jnp.int32, (TOK, HD), 1)
    sin_s[...] = jnp.where(lanes < HD // 2, -jnp.sin(angles), jnp.sin(angles))
    keep = jnp.max(jnp.where((lanes >= 1) & (lanes <= TILES), meta[...], 0.0), axis=1, keepdims=True)
    for i in range(2):
        fac[i] = jnp.where(keep > 0.0, jnp.tanh(jnp.full((TOK, HW), xg[i], F32)), 0.0)
    for k in range(AGC):
        ag(1, k).wait_recv()
        ag(2, k).start()
        if k == AGC - 2:
            load_v.wait()
            for j in range(VGROUP[1]):
                vcross(j).start()
    refill(-RING, 0, 560 - RING, 0)
    norm_rows(cross * OWN, OWN, 0)

    landed(0, OWN * KT, ag_r.at[5])
    norm_rows(diag * OWN, OWN, 0)
    vown().start()

    def rope(v):
        return (v * cos_s[...] + pltpu.roll(v, HD // 2, 1) * sin_s[...]).astype(BF16)

    at = spot("qkv_a", 0)
    landed(at, 8 * D, wsem.at[0])
    landed(at + 8 * D, 6 * D, wsem.at[1])
    r = mm(xn[...], panels(at, D, D, 8))
    for i in range(8):
        act[:, q_cols(i)] = rope(r[:, i * HD:(i + 1) * HD])
    r = mm(xn[...], panels(at + 8 * D, D, D, 6))
    for i in range(2):
        act[:, q_cols(8 + i)] = rope(r[:, i * HD:(i + 1) * HD])
        ks[i] = rope(r[:, (2 + i) * HD:(3 + i) * HD])
        vs[i] = r[:, (4 + i) * HD:(5 + i) * HD].astype(BF16)
    refill(0, 560, 0, 560)

    causal = lax.rem(lax.broadcasted_iota(jnp.int32, (REP * TOK, TOK), 0), TOK) >= lax.broadcasted_iota(jnp.int32, (REP * TOK, TOK), 1)
    for g in range(GROUPS):
        scores = dot_nt(q_group(g), ks[g]) * (HD ** -0.5)
        mixed = mm(softmax_rows(jnp.where(causal, scores, MASK_VALUE)), vs[g]).astype(BF16)
        for i in range(REP):
            act[:, (g * REP + i) * HD:(g * REP + i + 1) * HD] = mixed[i * TOK:(i + 1) * TOK]

    def to_sib(n):
        return remote(pall.at[n, 1 - co], psib.at[n], ps_s, ps_r.at[n], sib)

    def to_cross(n, par, half):
        if half:
            rows = pl.ds(pl.multiple_of((1 - xi) * PAIR, PAIR), PAIR)
            return remote(pall.at[n, co, rows], crcv.at[par, n, rows], cs_s, cs_r.at[par, n], cross)
        return remote(pall.at[n, co], crcv.at[par, n], cs_s, cs_r.at[par, n], cross)

    def half_cols(n):
        return pl.ds(pl.multiple_of(n * CW + co * HW, HW), HW)

    def h_out(n):
        ref = hbuf.at[:, half_cols(n)]
        return remote(ref, ref, hh_s, hh_r.at[n], sib)

    def each(fn):
        lax.fori_loop(0, CH, lambda n, _: (fn(n), 0)[1], 0)

    def reduce_out(name, left, rows, pitch, par, half, early, lag, fill=None):
        first, units, _ = SEG[name]

        def pair_sum(n):
            to_sib(n).wait_recv()
            pall[n, co] = (pall[n, co].astype(F32) + psib[n].astype(F32)).astype(BF16)
            to_cross(n, par, half).start()

        def chunk(n):
            start = spot(name, n)
            landed(start, 4 * rows, wsem.at[SEMS[name] + n])
            part = mm(left[...], panels(start, rows, pitch, 4))
            part = part.astype(BF16)
            for k in range(2):
                if half:
                    blocks = [part[r:r + OWN, q:q + HW] for r in (OWN * k, PAIR + OWN * k) for q in (0, HW)]
                    pall[n, k] = jnp.concatenate(blocks, axis=0)
                else:
                    pall[n, k] = part[:, k * HW:(k + 1) * HW]
            to_sib(n).start()
            if fill is None:
                refill(first + n * units, first + (n + 1) * units, first, first + CH * units)
            else:
                fill(n)

            if early < lag:
                @pl.when(n == early)
                def _():
                    pair_sum(0)

            @pl.when(n >= (lag if early == lag else lag + 1))
            def _():
                pair_sum(n - lag)

        each(chunk)
        for n in range(CH - lag, CH):
            pair_sum(n)

    def finish(par, factor, gain):
        def squares(v):
            v = v.astype(F32)
            v = v * v
            ssq[...] += v[:, :HD] + v[:, HD:]

        def absorb(n):
            h_out(n).wait_recv()
            squares(hbuf[:, pl.ds(pl.multiple_of(n * CW + (1 - co) * HW, HW), HW)])

        def chunk(n):
            to_cross(n, par, False).wait_recv()
            total = pall[n, co].astype(F32) + crcv[par, n].astype(F32)
            if factor is not None:
                total = fac[factor] * total
            cols = half_cols(n)
            fresh = (hbuf[:, cols].astype(F32) + total).astype(BF16)
            hbuf[:, cols] = fresh
            h_out(n).start()
            squares(fresh)

        ssq[...] = jnp.zeros_like(ssq)
        each(chunk)
        each(absorb)
        ssq[...] = jnp.broadcast_to(lax.rsqrt(jnp.sum(ssq[...], axis=1, keepdims=True) * (1.0 / D) + NORM_EPS), (TOK, HD))

        def block(b, _):
            rows = pl.ds(pl.multiple_of(b * SUB, SUB), SUB)
            xn[rows, :] = (hbuf[rows, :].astype(F32) * ssq[rows, 0:1] * gains[gain:gain + 1, :]).astype(BF16)
            return 0

        lax.fori_loop(0, TOK // SUB, block, 0)

        for sem in (hh_s, ps_s, cs_s):
            landed(0, CH * 2 * TOK, sem)

    def gate_up(name):
        first = SEG[name][0]

        def pairs(j, count):
            spots = [panel_spot(name, j * 2 + p) for p in range(2 * count)]
            for p in range(count):
                landed(spots[p * 2], 2 * D, wsem.at[SEMS[name] + lax.rem(j + p, GU_SEMS)])
            part = mm(xn[...], panel_set(spots, D))
            for p in range(count):
                gate = part[:, p * HW:p * HW + HD]
                up = part[:, p * HW + HD:p * HW + HW]
                act[:, pl.ds(pl.multiple_of((j + p) * HD, HD), HD)] = (jax.nn.silu(gate) * up).astype(BF16)
            refill(first + j * 80, first + (j + count) * 80, first, first + 2160, ("gu_a", "d_a"))

        lax.fori_loop(0, 6, lambda i, _: (pairs(i * 4, 4), 0)[1], 0)
        pairs(jnp.int32(24), 3)

    landed(0, 3 * OWN * KT, ag_s)
    reduce_out("o_a", act.at[:, 0:HEADS * HD], QW, QW, 0, False, 2, 2)
    for k in range(5, 14):
        vcross(k).start()
    finish(0, None, 1)
    relay_vision(0)
    gate_up("gu_a")

    def fill_late(n):
        for when, name in ((2, "kv_b"), (CH // 2, "q_b")):
            @pl.when(n == when)
            def _(name=name):
                start_all(name)

    reduce_out("d_a", act, FF, 30 * UNIT, 1, False, 1, 2, fill_late)
    for k in range(14, VCH):
        vcross(k).start()

    kv_at = spot("kv_b", 0)

    def kv_rows(states, spots):
        part = mm(states, panels(kv_at, D, D, 4))
        done = 0
        for rows, count in spots:
            piece = part[done:done + count]
            for g in range(GROUPS):
                kb[g, rows, :] = head_norm(piece[:, g * HD:(g + 1) * HD], k_gain).astype(BF16)
                vb[g, rows, :] = piece[:, (2 + g) * HD:(3 + g) * HD].astype(BF16)
            done += count

    def block_rows(b, start, count):
        return pl.ds(pl.multiple_of(b * TOK + start, SUB), count)

    landed(kv_at, 4 * D, wsem.at[SEMS["kv_b"]])
    vown().wait_recv()

    def near(i, _):
        b = me + i * (sib - me)
        kv_rows(vbuf[b], [(block_rows(b, 0, TOK), TOK)])
        return 0

    def far(i, _):
        b = cross + i * (diag - cross)
        kv_rows(vbuf[b, 0:EARLY, :], [(block_rows(b, 0, EARLY), EARLY)])
        return 0

    lax.fori_loop(0, 2, near, 0)
    relay_vision(1)
    refill(0, 4320, 0, 4320, ("o_b", "gu_b"))
    for g in range(2):
        landed(0, (VGROUP[g + 1] - VGROUP[g]) * 320, vr_r.at[g])
    lax.fori_loop(0, 2, far, 0)
    finish(1, None, 2)
    sprev[...] = ssq[...]

    q_spots = [panel_spot("q_b", j) for j in range(HEADS)]
    for i in range(2):
        landed(q_spots[i * 5], 5 * D, wsem.at[SEMS["q_b"] + i])
    for g in range(GROUPS):
        if g == 1:
            relay_vision(2)
        r = mm(xn[...], panel_set(q_spots[g * REP:(g + 1) * REP], D))
        for i in range(REP):
            act[:, q_cols(g * REP + i)] = head_norm(r[:, i * HD:(i + 1) * HD], q_gain).astype(BF16)
    refill(4320, 4720, 4320, 4720)
    landed(0, (VGROUP[3] - VGROUP[2]) * 320, vr_r.at[2])
    rest = TOK - EARLY
    kv_rows(jnp.concatenate([vbuf[cross, EARLY:, :], vbuf[diag, EARLY:, :]], axis=0),
            [(block_rows(b, EARLY, rest), rest) for b in (cross, diag)])
    refill(4720, 4880, 4720, 4880)

    for i in range(HEADS):
        scores = dot_nt(act[:, q_cols(i)], kb[i // REP]) * (HD ** -0.5)
        facc[2 * i] = scores[:, :HW]
        facc[2 * i + 1] = scores[:, HW:]

    def soft(b, _):
        rows = pl.ds(pl.multiple_of(b * OWN, OWN), OWN)
        seen = [jnp.broadcast_to(meta[rows, j + 1:j + 2], (OWN, HD)) > 0.0 for j in range(TILES)]
        for i in range(HEADS):
            parts = [facc[2 * i + j // 2, rows, j % 2 * HD:(j % 2 + 1) * HD] for j in range(TILES)]
            weights = softmax_rows(jnp.concatenate([jnp.where(m, v, MASK_VALUE) for m, v in zip(seen, parts)], axis=1))
            pall[i, 0, rows] = weights[:, :HW]
            pall[i, 1, rows] = weights[:, HW:]
        return 0

    lax.fori_loop(0, TOK // OWN, soft, 0)
    for g in range(GROUPS):
        heads = range(g * REP, (g + 1) * REP)
        mixed = sum(mm(jnp.concatenate([pall[i, p] for i in heads], axis=0), vb[g, p * HW:(p + 1) * HW, :]) for p in range(2)).astype(BF16)
        for n, i in enumerate(heads):
            act[:, i * HD:(i + 1) * HD] = mixed[n * TOK:(n + 1) * TOK]

    reduce_out("o_b", act.at[:, 0:HEADS * HD], QW, QW, 0, False, 2, 3)
    def finish_gate_up():
        first = SEG["gu_b"][0]

        def take(v, cols):
            v = v.astype(F32)
            sq = v * v
            ssq[...] += sq[:, :HD] + sq[:, HD:]
            xn[:, cols] = (v * sprev[:, 0:1] * gains[3:4, cols]).astype(BF16)

        def absorb(n):
            h_out(n).wait_recv()
            cols = pl.ds(pl.multiple_of(n * CW + (1 - co) * HW, HW), HW)
            take(hbuf[:, cols], cols)

        def own(n):
            to_cross(n, 0, False).wait_recv()
            cols = half_cols(n)
            total = fac[0] * (pall[n, co].astype(F32) + crcv[0, n].astype(F32))
            fresh = (hbuf[:, cols].astype(F32) + total).astype(BF16)
            hbuf[:, cols] = fresh
            h_out(n).start()
            take(fresh, cols)

        def products(n, store):
            at = spot("gu_b", n)
            left = xn[:, pl.ds(pl.multiple_of(n * CW, CW), CW)]
            for p in range(0, FF // HD, 4):
                count = min(4, FF // HD - p)
                part = mm(left, panel_set([at + (p * 2 + j) * CW for j in range(2 * count)], CW))
                for q in range(count):
                    store(p + q, part[:, q * HW:(q + 1) * HW])

        def arrive(n):
            landed(spot("gu_b", n), FF // PAIR * CW, wsem.at[SEMS["gu_b"] + n])

        def add(p, part):
            facc[p] += part

        def middle(n):
            absorb(n)
            arrive(n)
            products(n, add)

            refill(first + n * 240, first + (n + 1) * 240, first, first + 2160)

        def step(n):
            own(n)

            @pl.when(n >= 1)
            def _():
                middle(n - 1)

        ssq[...] = jnp.zeros_like(ssq)
        facc[...] = jnp.zeros_like(facc)
        each(step)
        last_n = jnp.int32(CH - 1)
        absorb(last_n)
        arrive(last_n)
        scale = lax.rsqrt(jnp.sum(ssq[...], axis=1, keepdims=True) * (1.0 / D) + NORM_EPS)
        ssq[...] = jnp.broadcast_to(scale, (TOK, HD)) / sprev[...]

        def activate(p, part):
            both = facc[p] + part
            act[:, p * HD:(p + 1) * HD] = (jax.nn.silu(both[:, :HD] * ssq[...]) * (both[:, HD:] * ssq[...])).astype(BF16)

        products(last_n, activate)
        refill(first + 2160, first + 2400, first + 2160, first + 2400)

        for sem in (hh_s, ps_s, cs_s):
            landed(0, CH * 2 * TOK, sem)

    finish_gate_up()
    vown().wait_send()
    landed(0, TOK * KT, vx_s)
    landed(0, TOK * KT, vr_s)
    reduce_out("d_b", act, FF, 30 * UNIT, 1, True, 2, 2)

    chip_rows = pl.ds(pl.multiple_of(xi * PAIR, PAIR), PAIR)

    def last(n):
        to_cross(n, 1, True).wait_recv()
        total = pall[n, co, chip_rows].astype(F32) + crcv[1, n, chip_rows].astype(F32)
        for q in range(2):
            cols = pl.ds(pl.multiple_of(n * CW + q * HW, HW), HW)
            xn[0:OWN, cols] = (hbuf[own_rows, cols].astype(F32) + fac[1, own_rows] * total[q * OWN:(q + 1) * OWN]).astype(BF16)
        cols = pl.ds(pl.multiple_of(n * CW, CW), CW)
        pltpu.make_async_copy(xn.at[0:OWN, cols], out.at[0, :, cols], lsem.at[2]).start()

    each(last)
    landed(0, CH * 2 * TOK, ps_s)
    landed(0, CH * TOK, cs_s)
    landed(0, 3 * PAIR, mt_s)
    landed(0, OWN * KT, lsem.at[2])


def solution(mesh):
    act_spec = P('dp', 'tp', None)
    col_spec = P(None, 'tp')
    row_spec = P('tp', None)
    layer_a = (P(), col_spec, col_spec, col_spec, row_spec, P(), col_spec, col_spec, row_spec)
    layer_b = (P(), col_spec, P(), col_spec, col_spec, P(), row_spec, P(), col_spec, col_spec, row_spec, P())
    in_specs = (act_spec, act_spec, P('dp', 'tp'), act_spec) + layer_a + layer_b

    def body(hidden, vision, positions, tile_mask, ln1_a, wq_a, wk_a, wv_a, wo_a, ln2_a, wg_a, wu_a, wd_a, ln1_b, wq_b, q_norm, wk_b, wv_b, k_norm, wo_b, ln2_b, wg_b, wu_b, wd_b, xgates):
        freq = rope_table(HD)
        freq = jnp.asarray(np.concatenate([freq, freq])[None, :])
        lns = [g.reshape(D // HD, HD) for g in (ln1_a, ln2_a, ln1_b, ln2_b)]
        heads = [g.reshape(1, HD) for g in (q_norm, k_norm)]
        vmem = pl.BlockSpec(memory_space=pltpu.VMEM)
        hbm = pl.BlockSpec(memory_space=pl.ANY)
        dma = pltpu.SemaphoreType.DMA
        return pl.pallas_call(
            kernel,
            out_shape=jax.ShapeDtypeStruct((1, OWN, D), BF16),
            in_specs=[vmem] * 3 + [pl.BlockSpec(memory_space=pltpu.SMEM)] + [vmem] * 6 + [hbm] * SUB,
            out_specs=hbm,
            scratch_shapes=[
                pltpu.VMEM((RING * UNIT, HD), BF16),
                pltpu.VMEM((TOK, D), BF16),
                pltpu.VMEM((TOK, D), BF16),
                pltpu.VMEM((4, TOK, D), BF16),
                pltpu.VMEM((4, D), F32),
                pltpu.VMEM((TOK, HD), F32),
                pltpu.VMEM((TOK, HD), F32),
                pltpu.VMEM((TOK, HD), F32),
                pltpu.VMEM((2, TOK, HW), F32),
                pltpu.VMEM((GROUPS, TOK, HD), BF16),
                pltpu.VMEM((GROUPS, TOK, HD), BF16),
                pltpu.VMEM((GROUPS, 4 * TOK, HD), BF16),
                pltpu.VMEM((GROUPS, 4 * TOK, HD), BF16),
                pltpu.VMEM((TOK, FF), BF16),
                pltpu.VMEM((CH, 2, TOK, HW), BF16),
                pltpu.VMEM((CH, TOK, HW), BF16),
                pltpu.VMEM((2, CH, TOK, HW), BF16),
                pltpu.VMEM((TOK, HD), F32),
                pltpu.VMEM((TOK, HD), F32),
                pltpu.VMEM((FF // HD, TOK, HW), F32),
                dma((NSEM,)), dma((3,)),
                dma(()), dma((6,)),
                dma(()), dma(()),
                dma(()), dma((3,)),
                dma(()), dma((3,)),
                dma(()), dma(()),
                dma(()), dma((CH,)),
                dma(()), dma((2, CH)),
                dma(()), dma((CH,)),
            ],
            compiler_params=pltpu.CompilerParams(collective_id=0, has_side_effects=True, vmem_limit_bytes=67043328),
        )(positions, jnp.swapaxes(tile_mask, 1, 2), freq, xgates, *lns, *heads, hidden, vision, wq_a, wk_a, wv_a, wo_a, wg_a, wu_a, wd_a, wq_b, wk_b, wv_b, wo_b, wg_b, wu_b, wd_b)

    return jax.shard_map(body, mesh=mesh, in_specs=in_specs, out_specs=act_spec, check_vma=False)
```

```python
import math

import jax
import jax.numpy as jnp
import numpy as np
from jax import lax
from jax.experimental import pallas as pl
from jax.experimental.pallas import tpu as pltpu
from jax.sharding import PartitionSpec as P

ROPE_THETA = 500000.0
ROPE_FACTOR = 8.0
LOW_FACTOR = 1.0
HIGH_FACTOR = 4.0
ORIG_CONTEXT = 8192.0
NORM_EPS = 1e-5
MASK_VALUE = -1e30
MESH = pl.DeviceIdType.MESH
F32 = jnp.float32
BF16 = jnp.bfloat16

D = 5120
TOK = 128
HD = 128
HEADS = 10
GROUPS = 2
REP = 5
FF = 3456
TILES = 4
CH = 10
CW = D // CH
HW = CW // 2
OWN = 32
PAIR = 64
KT = 40
QW = 1280
SUB = 16
UNIT = 128
RING = 1440
AGC = 4
VCH = 16
VGROUP = (0, 4, 14, 16)
EARLY = 112

SEG = {
    "qkv_a": (0, 560, 1),
    "o_a": (560, 40, 10),
    "gu_a": (960, 80, 27),
    "d_a": (3120, 120, 10),
    "q_b": (4320, 40, 10),
    "kv_b": (4720, 160, 1),
    "o_b": (4880, 40, 10),
    "gu_b": (5280, 240, 10),
    "d_b": (7680, 120, 10),
}
SEMS = {"qkv_a": 0, "q_b": 0, "o_a": 2, "o_b": 2, "d_a": 12, "d_b": 12, "gu_a": 22, "gu_b": 22, "kv_b": 40}
NSEM = 41
GU_SEMS = 18


def rope_table(head_dim):
    low_wave = ORIG_CONTEXT / LOW_FACTOR
    high_wave = ORIG_CONTEXT / HIGH_FACTOR
    freq_list = []
    for freq_idx in range(head_dim // 2):
        base_freq = 1.0 / (ROPE_THETA ** (2.0 * freq_idx / head_dim))
        wave_len = 2.0 * math.pi / base_freq
        if wave_len > low_wave:
            freq_list.append(base_freq / ROPE_FACTOR)
        elif wave_len < high_wave:
            freq_list.append(base_freq)
        else:
            smooth = (ORIG_CONTEXT / wave_len - LOW_FACTOR) / (HIGH_FACTOR - LOW_FACTOR)
            freq_list.append((1.0 - smooth) * base_freq / ROPE_FACTOR + smooth * base_freq)
    return np.array(freq_list, dtype=np.float32)


def head_norm(values, gain):
    mean_sq = jnp.mean(values * values, axis=-1, keepdims=True)
    return values * lax.rsqrt(mean_sq + NORM_EPS) * gain


def softmax_rows(scores):
    top = jnp.max(scores, axis=-1, keepdims=True)
    weights = jnp.exp(scores - top)
    return (weights * (1.0 / jnp.sum(weights, axis=-1, keepdims=True))).astype(BF16)


def dot_nt(left, right):
    return lax.dot_general(left, right, (((1,), (1,)), ((), ())), preferred_element_type=F32)


def kernel(pos, tmask, freq, xg, ln1_a, ln2_a, ln1_b, ln2_b, qn, kn, hid, vis, wq_a, wk_a, wv_a, wo_a, wg_a, wu_a, wd_a, wq_b, wk_b, wv_b, wo_b, wg_b, wu_b, wd_b, out,
           ring, hbuf, xn, vbuf, gains, meta, cos_s, sin_s, fac, ks, vs, kb, vb, act, pall, psib, crcv, ssq, sprev, facc,
           wsem, lsem, ag_s, ag_r, mt_s, mt_r, vx_s, vx_r, vr_s, vr_r, vo_s, vo_r, ps_s, ps_r, cs_s, cs_r, hh_s, hh_r):
    me = lax.axis_index("tp")
    xi = lax.div(me, 2)
    co = lax.rem(me, 2)
    sib = xi * 2 + 1 - co
    cross = (1 - xi) * 2 + co
    diag = (1 - xi) * 2 + 1 - co

    def remote(src, dst, ssem, rsem, dev):
        return pltpu.make_async_remote_copy(src_ref=src, dst_ref=dst, send_sem=ssem, recv_sem=rsem, device_id={"tp": dev}, device_id_type=MESH)

    def spot(name, j):
        first, units, _ = SEG[name]
        return lax.rem(first + j * units, RING) * UNIT

    def panel_spot(name, j):
        return lax.rem(SEG[name][0] + j * KT, RING) * UNIT

    def put(weight, rows, col, at, sem, first=0):
        pltpu.make_async_copy(weight.at[pl.ds(first, rows), pl.ds(pl.multiple_of(col * HD, HD), HD)], ring.at[pl.ds(pl.multiple_of(at, HD), rows)], sem).start()

    def start_group(name, j):
        at = spot(name, j)
        base = SEMS[name]
        if name[:2] == "o_":
            for p in range(4):
                put(wo_a if name == "o_a" else wo_b, QW, j * 4 + p, at + p * QW, wsem.at[base + j])
        elif name == "gu_b":
            def pairs(i, _):
                for q in range(9):
                    for p, w in enumerate((wg_b, wu_b)):
                        put(w, CW, i * 9 + q, at + (i * 18 + q * 2 + p) * CW, wsem.at[base + j], pl.multiple_of(j * CW, CW))
                return 0
            lax.fori_loop(0, FF // HD // 9, pairs, 0)
        elif name == "gu_a":
            put(wg_a, D, j, at, wsem.at[base + lax.rem(j, GU_SEMS)])
            put(wu_a, D, j, at + D, wsem.at[base + lax.rem(j, GU_SEMS)])
        elif name[:2] == "d_":
            for p in range(4):
                put(wd_a if name == "d_a" else wd_b, FF, j * 4 + p, at + p * 30 * UNIT, wsem.at[base + j])
        elif name == "q_b":
            put(wq_b, D, j, at, wsem.at[base + lax.div(j, 5)])
        elif name == "kv_b":
            for p, w in enumerate((wk_b, wk_b, wv_b, wv_b)):
                put(w, D, p % 2, at + p * D, wsem.at[base])
        else:
            for p in range(14):
                w = wq_a if p < 10 else (wk_a if p < 12 else wv_a)
                put(w, D, p if p < 10 else p % 2, at + p * D, wsem.at[base + p // 8])

    def ready(name, freed):
        first, units, count = SEG[name]
        if isinstance(freed, int):
            return min(max((freed + RING - first) // units, 0), count)
        return jnp.minimum(jnp.maximum(lax.div(freed + RING - first + 100 * units, units) - 100, 0), count)

    def refill(before, after, low, high, names=tuple(SEG)):
        for name in names:
            first, units, count = SEG[name]
            if first + units > high + RING or first + units * count <= low + RING:
                continue
            lo, hi = ready(name, before), ready(name, after)
            if isinstance(lo, int) and isinstance(hi, int) and lo >= hi:
                continue
            lax.fori_loop(lo, hi, lambda j, _, name=name: (start_group(name, j), 0)[1], 0)

    def start_all(name):
        lax.fori_loop(0, SEG[name][2], lambda j, _: (start_group(name, j), 0)[1], 0)

    def landed(at, rows, sem):
        span = ring.at[pl.ds(pl.multiple_of(at, HD), rows)]
        pltpu.make_async_copy(span, span, sem).wait()

    def panel_set(spots, rows):
        return jnp.concatenate([ring[pl.ds(pl.multiple_of(at, HD), rows), :] for at in spots], axis=1)

    def panels(at, rows, pitch, count):
        return jnp.concatenate([ring[pl.ds(pl.multiple_of(at + p * pitch, HD), rows), :] for p in range(count)], axis=1)

    def mm(left, right):
        return jnp.dot(left, right, preferred_element_type=F32)

    def q_cols(i):
        start = (HEADS + i) * HD
        return pl.ds(start if isinstance(i, int) else pl.multiple_of(start, HD), HD)

    def q_group(g):
        return jnp.concatenate([act[:, q_cols(g * REP + i)] for i in range(REP)], axis=0)

    own_rows = pl.ds(pl.multiple_of(me * OWN, OWN), OWN)
    load_h = pltpu.make_async_copy(hid.at[0], hbuf.at[own_rows], lsem.at[0])
    load_h.start()
    load_v = pltpu.make_async_copy(vis.at[0], vbuf.at[me], lsem.at[1])
    barrier = pltpu.get_barrier_semaphore()
    for dev in (sib, cross, diag):
        pl.semaphore_signal(barrier, inc=1, device_id={"tp": dev}, device_id_type=MESH)
    row_i = lax.broadcasted_iota(jnp.int32, (OWN, HD), 0)
    lane_i = lax.broadcasted_iota(jnp.int32, (OWN, HD), 1)
    pos_row = jnp.concatenate([jnp.broadcast_to(pos[...].astype(F32), (OWN, OWN)), jnp.zeros((OWN, 96), F32)], axis=1)
    pos_col = jnp.sum(jnp.where(row_i == lane_i, pos_row, 0.0), axis=1, keepdims=True)
    own_meta = jnp.where(lane_i == 0, pos_col, 0.0)
    for j in range(TILES):
        tm_row = jnp.concatenate([jnp.broadcast_to(tmask[0, j:j + 1, :].astype(F32), (OWN, OWN)), jnp.zeros((OWN, 96), F32)], axis=1)
        tm_col = jnp.sum(jnp.where(row_i == lane_i, tm_row, 0.0), axis=1, keepdims=True)
        own_meta = jnp.where(lane_i == j + 1, tm_col, own_meta)
    meta[own_rows, :] = own_meta
    load_h.wait()
    pl.semaphore_wait(barrier, 3)

    def ag(kind, k):
        cols = pl.ds(k * (D // AGC), D // AGC)
        rows = pl.ds(pl.multiple_of((cross if kind == 2 else me) * OWN, OWN), OWN)
        ref = hbuf.at[rows, cols]
        return remote(ref, ref, ag_s, ag_r.at[(4, k, 5)[kind]], cross if kind == 1 else sib)

    def vown():
        return remote(vbuf.at[me], vbuf.at[me], vo_s, vo_r, sib)

    def vpiece(owner, k):
        return vbuf.at[owner, pl.ds(k // 2 * SUB, SUB), pl.ds(k % 2 * (D // 2), D // 2)]

    def vgroup(k):
        return 0 if k < VGROUP[1] else (1 if k < VGROUP[2] else 2)

    def vcross(k):
        return remote(vpiece(me, k), vpiece(me, k), vx_s, vx_r.at[vgroup(k)], cross)

    def vrelay(k):
        return remote(vpiece(cross, k), vpiece(cross, k), vr_s, vr_r.at[vgroup(k)], sib)

    def relay_vision(g):
        landed(0, (VGROUP[g + 1] - VGROUP[g]) * 320, vx_r.at[g])
        for k in range(VGROUP[g], VGROUP[g + 1]):
            vrelay(k).start()

    for k in range(AGC):
        ag(0, k).start()
    for k in range(AGC):
        ag(1, k).start()
    metas = [remote(meta.at[own_rows], meta.at[own_rows], mt_s, mt_r, dev) for dev in (sib, cross, diag)]
    for m in metas:
        m.start()
    load_v.start()
    start_group("qkv_a", 0)

    for i, ln in enumerate((ln1_a, ln2_a, ln1_b, ln2_b)):
        for p in range(D // HD):
            gains[i:i + 1, p * HD:(p + 1) * HD] = ln[p:p + 1, :].astype(F32)
    q_gain = qn[...].astype(F32)
    k_gain = kn[...].astype(F32)

    def norm_rows(first, count, gain):
        def block(b, _):
            rows = pl.ds(pl.multiple_of(first + b * SUB, SUB), SUB)
            v = hbuf[rows, :].astype(F32)
            scale = lax.rsqrt(jnp.mean(v * v, axis=-1, keepdims=True) + NORM_EPS)
            xn[rows, :] = (v * scale * gains[gain:gain + 1, :]).astype(BF16)
            return 0
        lax.fori_loop(0, count // SUB, block, 0)

    norm_rows(me * OWN, OWN, 0)
    landed(0, OWN * KT, ag_r.at[4])
    norm_rows(sib * OWN, OWN, 0)
    landed(0, 3 * PAIR, mt_r)
    angles = meta[:, 0:1] * freq[...]
    cos_s[...] = jnp.cos(angles)
    lanes = lax.broadcasted_iota(jnp.int32, (TOK, HD), 1)
    sin_s[...] = jnp.where(lanes < HD // 2, -jnp.sin(angles), jnp.sin(angles))
    keep = jnp.max(jnp.where((lanes >= 1) & (lanes <= TILES), meta[...], 0.0), axis=1, keepdims=True)
    for i in range(2):
        fac[i] = jnp.where(keep > 0.0, jnp.tanh(jnp.full((TOK, HW), xg[i], F32)), 0.0)
    for k in range(AGC):
        ag(1, k).wait_recv()
        ag(2, k).start()
        if k == AGC - 2:
            load_v.wait()
            for j in range(VGROUP[1]):
                vcross(j).start()
    refill(-RING, 0, 560 - RING, 0)
    norm_rows(cross * OWN, OWN, 0)

    landed(0, OWN * KT, ag_r.at[5])
    norm_rows(diag * OWN, OWN, 0)
    vown().start()

    def rope(v):
        return (v * cos_s[...] + pltpu.roll(v, HD // 2, 1) * sin_s[...]).astype(BF16)

    at = spot("qkv_a", 0)
    landed(at, 8 * D, wsem.at[0])
    landed(at + 8 * D, 6 * D, wsem.at[1])
    r = mm(xn[...], panels(at, D, D, 8))
    for i in range(8):
        act[:, q_cols(i)] = rope(r[:, i * HD:(i + 1) * HD])
    r = mm(xn[...], panels(at + 8 * D, D, D, 6))
    for i in range(2):
        act[:, q_cols(8 + i)] = rope(r[:, i * HD:(i + 1) * HD])
        ks[i] = rope(r[:, (2 + i) * HD:(3 + i) * HD])
        vs[i] = r[:, (4 + i) * HD:(5 + i) * HD].astype(BF16)
    refill(0, 560, 0, 560)

    causal = lax.rem(lax.broadcasted_iota(jnp.int32, (REP * TOK, TOK), 0), TOK) >= lax.broadcasted_iota(jnp.int32, (REP * TOK, TOK), 1)
    for g in range(GROUPS):
        scores = dot_nt(q_group(g), ks[g]) * (HD ** -0.5)
        mixed = mm(softmax_rows(jnp.where(causal, scores, MASK_VALUE)), vs[g]).astype(BF16)
        for i in range(REP):
            act[:, (g * REP + i) * HD:(g * REP + i + 1) * HD] = mixed[i * TOK:(i + 1) * TOK]

    def to_sib(n):
        return remote(pall.at[n, 1 - co], psib.at[n], ps_s, ps_r.at[n], sib)

    def to_cross(n, par, half):
        if half:
            rows = pl.ds(pl.multiple_of((1 - xi) * PAIR, PAIR), PAIR)
            return remote(pall.at[n, co, rows], crcv.at[par, n, rows], cs_s, cs_r.at[par, n], cross)
        return remote(pall.at[n, co], crcv.at[par, n], cs_s, cs_r.at[par, n], cross)

    def half_cols(n):
        return pl.ds(pl.multiple_of(n * CW + co * HW, HW), HW)

    def h_out(n):
        ref = hbuf.at[:, half_cols(n)]
        return remote(ref, ref, hh_s, hh_r.at[n], sib)

    def each(fn):
        lax.fori_loop(0, CH, lambda n, _: (fn(n), 0)[1], 0)

    def reduce_out(name, left, rows, pitch, par, half, early, lag, fill=None):
        first, units, _ = SEG[name]

        def pair_sum(n):
            to_sib(n).wait_recv()
            pall[n, co] = (pall[n, co].astype(F32) + psib[n].astype(F32)).astype(BF16)
            to_cross(n, par, half).start()

        def chunk(n):
            start = spot(name, n)
            landed(start, 4 * rows, wsem.at[SEMS[name] + n])
            part = mm(left[...], panels(start, rows, pitch, 4))
            part = part.astype(BF16)
            for k in range(2):
                if half:
                    blocks = [part[r:r + OWN, q:q + HW] for r in (OWN * k, PAIR + OWN * k) for q in (0, HW)]
                    pall[n, k] = jnp.concatenate(blocks, axis=0)
                else:
                    pall[n, k] = part[:, k * HW:(k + 1) * HW]
            to_sib(n).start()
            if fill is None:
                refill(first + n * units, first + (n + 1) * units, first, first + CH * units)
            else:
                fill(n)

            if early < lag:
                @pl.when(n == early)
                def _():
                    pair_sum(0)

            @pl.when(n >= (lag if early == lag else lag + 1))
            def _():
                pair_sum(n - lag)

        each(chunk)
        for n in range(CH - lag, CH):
            pair_sum(n)

    def finish(par, factor, gain):
        def squares(v):
            v = v.astype(F32)
            v = v * v
            ssq[...] += v[:, :HD] + v[:, HD:]

        def absorb(n):
            h_out(n).wait_recv()
            squares(hbuf[:, pl.ds(pl.multiple_of(n * CW + (1 - co) * HW, HW), HW)])

        def chunk(n):
            to_cross(n, par, False).wait_recv()
            total = pall[n, co].astype(F32) + crcv[par, n].astype(F32)
            if factor is not None:
                total = fac[factor] * total
            cols = half_cols(n)
            fresh = (hbuf[:, cols].astype(F32) + total).astype(BF16)
            hbuf[:, cols] = fresh
            h_out(n).start()
            squares(fresh)

        ssq[...] = jnp.zeros_like(ssq)
        each(chunk)
        each(absorb)
        ssq[...] = jnp.broadcast_to(lax.rsqrt(jnp.sum(ssq[...], axis=1, keepdims=True) * (1.0 / D) + NORM_EPS), (TOK, HD))

        def block(b, _):
            rows = pl.ds(pl.multiple_of(b * SUB, SUB), SUB)
            xn[rows, :] = (hbuf[rows, :].astype(F32) * ssq[rows, 0:1] * gains[gain:gain + 1, :]).astype(BF16)
            return 0

        lax.fori_loop(0, TOK // SUB, block, 0)

        for sem in (hh_s, ps_s, cs_s):
            landed(0, CH * 2 * TOK, sem)

    def gate_up(name):
        first = SEG[name][0]

        def pairs(j, count):
            spots = [panel_spot(name, j * 2 + p) for p in range(2 * count)]
            for p in range(count):
                landed(spots[p * 2], 2 * D, wsem.at[SEMS[name] + lax.rem(j + p, GU_SEMS)])
            part = mm(xn[...], panel_set(spots, D))
            for p in range(count):
                gate = part[:, p * HW:p * HW + HD]
                up = part[:, p * HW + HD:p * HW + HW]
                act[:, pl.ds(pl.multiple_of((j + p) * HD, HD), HD)] = (jax.nn.silu(gate) * up).astype(BF16)
            refill(first + j * 80, first + (j + count) * 80, first, first + 2160, ("gu_a", "d_a"))

        lax.fori_loop(0, 6, lambda i, _: (pairs(i * 4, 4), 0)[1], 0)
        pairs(jnp.int32(24), 3)

    landed(0, 3 * OWN * KT, ag_s)
    reduce_out("o_a", act.at[:, 0:HEADS * HD], QW, QW, 0, False, 2, 2)
    for k in range(VGROUP[1], VGROUP[2]):
        vcross(k).start()
    finish(0, None, 1)
    relay_vision(0)
    gate_up("gu_a")

    def fill_late(n):
        for when, name in ((2, "kv_b"), (CH // 2, "q_b")):
            @pl.when(n == when)
            def _(name=name):
                start_all(name)

    reduce_out("d_a", act, FF, 30 * UNIT, 1, False, 1, 2, fill_late)
    for k in range(14, VCH):
        vcross(k).start()

    kv_at = spot("kv_b", 0)

    def kv_rows(states, spots):
        part = mm(states, panels(kv_at, D, D, 4))
        done = 0
        for rows, count in spots:
            piece = part[done:done + count]
            for g in range(GROUPS):
                kb[g, rows, :] = head_norm(piece[:, g * HD:(g + 1) * HD], k_gain).astype(BF16)
                vb[g, rows, :] = piece[:, (2 + g) * HD:(3 + g) * HD].astype(BF16)
            done += count

    def block_rows(b, start, count):
        return pl.ds(pl.multiple_of(b * TOK + start, SUB), count)

    landed(kv_at, 4 * D, wsem.at[SEMS["kv_b"]])
    vown().wait_recv()

    def near(i, _):
        b = me + i * (sib - me)
        kv_rows(vbuf[b], [(block_rows(b, 0, TOK), TOK)])
        return 0

    def far(i, _):
        b = cross + i * (diag - cross)
        kv_rows(vbuf[b, 0:EARLY, :], [(block_rows(b, 0, EARLY), EARLY)])
        return 0

    lax.fori_loop(0, 2, near, 0)
    relay_vision(1)
    refill(0, 4320, 0, 4320, ("o_b", "gu_b"))
    for g in range(2):
        landed(0, (VGROUP[g + 1] - VGROUP[g]) * 320, vr_r.at[g])
    lax.fori_loop(0, 2, far, 0)
    finish(1, None, 2)
    sprev[...] = ssq[...]

    q_spots = [panel_spot("q_b", j) for j in range(HEADS)]
    for i in range(2):
        landed(q_spots[i * 5], 5 * D, wsem.at[SEMS["q_b"] + i])
    for g in range(GROUPS):
        if g == 1:
            relay_vision(2)
        r = mm(xn[...], panel_set(q_spots[g * REP:(g + 1) * REP], D))
        for i in range(REP):
            act[:, q_cols(g * REP + i)] = head_norm(r[:, i * HD:(i + 1) * HD], q_gain).astype(BF16)
    refill(4320, 4720, 4320, 4720)
    landed(0, (VGROUP[3] - VGROUP[2]) * 320, vr_r.at[2])
    rest = TOK - EARLY
    kv_rows(jnp.concatenate([vbuf[cross, EARLY:, :], vbuf[diag, EARLY:, :]], axis=0),
            [(block_rows(b, EARLY, rest), rest) for b in (cross, diag)])
    refill(4720, 4880, 4720, 4880)

    for i in range(HEADS):
        scores = dot_nt(act[:, q_cols(i)], kb[i // REP]) * (HD ** -0.5)
        facc[2 * i] = scores[:, :HW]
        facc[2 * i + 1] = scores[:, HW:]

    def soft(b, _):
        rows = pl.ds(pl.multiple_of(b * OWN, OWN), OWN)
        seen = [jnp.broadcast_to(meta[rows, j + 1:j + 2], (OWN, HD)) > 0.0 for j in range(TILES)]
        for i in range(HEADS):
            parts = [facc[2 * i + j // 2, rows, j % 2 * HD:(j % 2 + 1) * HD] for j in range(TILES)]
            weights = softmax_rows(jnp.concatenate([jnp.where(m, v, MASK_VALUE) for m, v in zip(seen, parts)], axis=1))
            pall[i, 0, rows] = weights[:, :HW]
            pall[i, 1, rows] = weights[:, HW:]
        return 0

    lax.fori_loop(0, TOK // OWN, soft, 0)
    for g in range(GROUPS):
        heads = range(g * REP, (g + 1) * REP)
        mixed = sum(mm(jnp.concatenate([pall[i, p] for i in heads], axis=0), vb[g, p * HW:(p + 1) * HW, :]) for p in range(2)).astype(BF16)
        for n, i in enumerate(heads):
            act[:, i * HD:(i + 1) * HD] = mixed[n * TOK:(n + 1) * TOK]

    reduce_out("o_b", act.at[:, 0:HEADS * HD], QW, QW, 0, False, 2, 3)
    def finish_gate_up():
        first = SEG["gu_b"][0]

        def take(v, cols):
            v = v.astype(F32)
            sq = v * v
            ssq[...] += sq[:, :HD] + sq[:, HD:]
            xn[:, cols] = (v * sprev[:, 0:1] * gains[3:4, cols]).astype(BF16)

        def absorb(n):
            h_out(n).wait_recv()
            cols = pl.ds(pl.multiple_of(n * CW + (1 - co) * HW, HW), HW)
            take(hbuf[:, cols], cols)

        def own(n):
            to_cross(n, 0, False).wait_recv()
            cols = half_cols(n)
            total = fac[0] * (pall[n, co].astype(F32) + crcv[0, n].astype(F32))
            fresh = (hbuf[:, cols].astype(F32) + total).astype(BF16)
            hbuf[:, cols] = fresh
            h_out(n).start()
            take(fresh, cols)

        def products(n, store):
            at = spot("gu_b", n)
            left = xn[:, pl.ds(pl.multiple_of(n * CW, CW), CW)]
            for p in range(0, FF // HD, 4):
                count = min(4, FF // HD - p)
                part = mm(left, panel_set([at + (p * 2 + j) * CW for j in range(2 * count)], CW))
                for q in range(count):
                    store(p + q, part[:, q * HW:(q + 1) * HW])

        def arrive(n):
            landed(spot("gu_b", n), FF // PAIR * CW, wsem.at[SEMS["gu_b"] + n])

        def add(p, part):
            facc[p] += part

        def middle(n):
            absorb(n)
            arrive(n)
            products(n, add)

            refill(first + n * 240, first + (n + 1) * 240, first, first + 2160)

        def step(n):
            own(n)

            @pl.when(n >= 1)
            def _():
                middle(n - 1)

        ssq[...] = jnp.zeros_like(ssq)
        facc[...] = jnp.zeros_like(facc)
        each(step)
        last_n = jnp.int32(CH - 1)
        absorb(last_n)
        arrive(last_n)
        scale = lax.rsqrt(jnp.sum(ssq[...], axis=1, keepdims=True) * (1.0 / D) + NORM_EPS)
        ssq[...] = jnp.broadcast_to(scale, (TOK, HD)) / sprev[...]

        def activate(p, part):
            both = facc[p] + part
            act[:, p * HD:(p + 1) * HD] = (jax.nn.silu(both[:, :HD] * ssq[...]) * (both[:, HD:] * ssq[...])).astype(BF16)

        products(last_n, activate)
        refill(first + 2160, first + 2400, first + 2160, first + 2400)

        for sem in (hh_s, ps_s, cs_s):
            landed(0, CH * 2 * TOK, sem)

    finish_gate_up()
    vown().wait_send()
    landed(0, TOK * KT, vx_s)
    landed(0, TOK * KT, vr_s)
    reduce_out("d_b", act, FF, 30 * UNIT, 1, True, 2, 2)

    chip_rows = pl.ds(pl.multiple_of(xi * PAIR, PAIR), PAIR)

    def last(n):
        to_cross(n, 1, True).wait_recv()
        total = pall[n, co, chip_rows].astype(F32) + crcv[1, n, chip_rows].astype(F32)
        for q in range(2):
            cols = pl.ds(pl.multiple_of(n * CW + q * HW, HW), HW)
            xn[0:OWN, cols] = (hbuf[own_rows, cols].astype(F32) + fac[1, own_rows] * total[q * OWN:(q + 1) * OWN]).astype(BF16)
        cols = pl.ds(pl.multiple_of(n * CW, CW), CW)
        pltpu.make_async_copy(xn.at[0:OWN, cols], out.at[0, :, cols], lsem.at[2]).start()

    each(last)
    landed(0, CH * 2 * TOK, ps_s)
    landed(0, CH * TOK, cs_s)
    landed(0, 3 * PAIR, mt_s)
    landed(0, OWN * KT, lsem.at[2])


def solution(mesh):
    act_spec = P('dp', 'tp', None)
    col_spec = P(None, 'tp')
    row_spec = P('tp', None)
    layer_a = (P(), col_spec, col_spec, col_spec, row_spec, P(), col_spec, col_spec, row_spec)
    layer_b = (P(), col_spec, P(), col_spec, col_spec, P(), row_spec, P(), col_spec, col_spec, row_spec, P())
    in_specs = (act_spec, act_spec, P('dp', 'tp'), act_spec) + layer_a + layer_b

    def body(hidden, vision, positions, tile_mask, ln1_a, wq_a, wk_a, wv_a, wo_a, ln2_a, wg_a, wu_a, wd_a, ln1_b, wq_b, q_norm, wk_b, wv_b, k_norm, wo_b, ln2_b, wg_b, wu_b, wd_b, xgates):
        freq = rope_table(HD)
        freq = jnp.asarray(np.concatenate([freq, freq])[None, :])
        lns = [g.reshape(D // HD, HD) for g in (ln1_a, ln2_a, ln1_b, ln2_b)]
        heads = [g.reshape(1, HD) for g in (q_norm, k_norm)]
        vmem = pl.BlockSpec(memory_space=pltpu.VMEM)
        hbm = pl.BlockSpec(memory_space=pl.ANY)
        dma = pltpu.SemaphoreType.DMA
        return pl.pallas_call(
            kernel,
            out_shape=jax.ShapeDtypeStruct((1, OWN, D), BF16),
            in_specs=[vmem] * 3 + [pl.BlockSpec(memory_space=pltpu.SMEM)] + [vmem] * 6 + [hbm] * SUB,
            out_specs=hbm,
            scratch_shapes=[
                pltpu.VMEM((RING * UNIT, HD), BF16),
                pltpu.VMEM((TOK, D), BF16),
                pltpu.VMEM((TOK, D), BF16),
                pltpu.VMEM((4, TOK, D), BF16),
                pltpu.VMEM((4, D), F32),
                pltpu.VMEM((TOK, HD), F32),
                pltpu.VMEM((TOK, HD), F32),
                pltpu.VMEM((TOK, HD), F32),
                pltpu.VMEM((2, TOK, HW), F32),
                pltpu.VMEM((GROUPS, TOK, HD), BF16),
                pltpu.VMEM((GROUPS, TOK, HD), BF16),
                pltpu.VMEM((GROUPS, 4 * TOK, HD), BF16),
                pltpu.VMEM((GROUPS, 4 * TOK, HD), BF16),
                pltpu.VMEM((TOK, FF), BF16),
                pltpu.VMEM((CH, 2, TOK, HW), BF16),
                pltpu.VMEM((CH, TOK, HW), BF16),
                pltpu.VMEM((2, CH, TOK, HW), BF16),
                pltpu.VMEM((TOK, HD), F32),
                pltpu.VMEM((TOK, HD), F32),
                pltpu.VMEM((FF // HD, TOK, HW), F32),
                dma((NSEM,)), dma((3,)),
                dma(()), dma((6,)),
                dma(()), dma(()),
                dma(()), dma((3,)),
                dma(()), dma((3,)),
                dma(()), dma(()),
                dma(()), dma((CH,)),
                dma(()), dma((2, CH)),
                dma(()), dma((CH,)),
            ],
            compiler_params=pltpu.CompilerParams(collective_id=0, has_side_effects=True, vmem_limit_bytes=67043328),
        )(positions, jnp.swapaxes(tile_mask, 1, 2), freq, xgates, *lns, *heads, hidden, vision, wq_a, wk_a, wv_a, wo_a, wg_a, wu_a, wd_a, wq_b, wk_b, wv_b, wo_b, wg_b, wu_b, wd_b)

    return jax.shard_map(body, mesh=mesh, in_specs=in_specs, out_specs=act_spec, check_vma=False)
```
